512 devices in a mesh: sub: 128 (over z, y, core), grp: 4 (over x).
Axes of the slice: x: 4, y: 8, z: 8, core: 2. Of those that a mesh axis runs over, the one named last changes fastest.
Arguments:
- schur: bfloat16 [128, 2048, 2048], P('sub', 'grp'), may hold values from -0.125 to 0.125
- rhs: float32 [128, 2048, 192], P('sub', 'grp'), may hold values from -6 to 6
- start: float32 [128, 2048, 192], P('sub', 'grp'), may hold values from -6 to 6
- project: bfloat16 [128, 32, 4096], P('sub', 'grp'), may hold values from -0.75 to 0.75
- coarse_basis: bfloat16 [128, 8, 2048], P('sub', None, 'grp'), may hold values from -0.375 to 0.375
- owner_of_face: int32 [128, 32, 1], replicated, may hold values from 0 to 4; in each aligned block of 32 rows (0 to 31, 32 to 63, ..., all dimensions but the last counted through in order) at most 8 rows name the same one
- mortar_of_face: int32 [128, 32], replicated, may hold values from 0 to 15
- mortar_order: int32 [128, 16], replicated, may hold values from 3 to 7
- subdomain_map: int32 [128], replicated, may hold values from 0 to 127, each once
- vertex_ids: int32 [128, 8], replicated, may hold values from 0 to 255, all different within a row
Outputs:
- solution: float32 [128, 2048, 192], P('sub', 'grp')
The draws below stay inside these ranges and needn't reach their ends.
Inputs may be any that keep to these rules, and one draw needn't show every extreme that they name: `owner_of_face`: the 32 faces of one subdomain name one offset at most 8 times. `mortar_of_face`: faces with the same owner and the same number lie on one mortar. `mortar_order`: row o holds the orders of the mortars owned by index o. `subdomain_map`: each subdomain once. `vertex_ids`: the 8 vertices of a subdomain differ; every vertex belongs to some subdomain.
All inputs are finite; a program needn't handle non-finite values.
Results may differ from the reference program's by a relative error of at most 0.0031.
Values may be sent and summed in bfloat16 or wider, within the bound.
A program may use at most 64 MiB of HBM per device.

```python
import math
import jax
import jax.numpy as jnp
import numpy as np
from jax import lax

DEG = 8
FPTS = 64
MODES = 64
FACES = 32
M = 2048
R = 192
NCV = 8
MORT_OWN = 16
ITERS = 2
REACH = 2
NB = 5
CAP = 8
SUBS = 128
NV = 256


def place_ends(result, key, smallest, largest):
    longest = result.shape.index(max(result.shape))
    spots = []
    for shift in (0, 1):
        where = [jax.random.randint(jax.random.fold_in(key, axis), (), 0, length) for axis, length in enumerate(result.shape)]
        where[longest] = (where[longest] + shift) % result.shape[longest]
        spots.append(tuple(where))
    return result.at[spots[0]].set(smallest).at[spots[1]].set(largest)


def shard_levels(own_key, extent, shards, low, high):
    level, own = 1.0, jax.random.fold_in(own_key, 6)
    for dim, shards_of in shards:
        steps = jnp.exp(jax.random.uniform(jax.random.fold_in(own, dim), (shards_of,), jnp.float32, low / len(shards), high / len(shards)))
        level = level * jnp.repeat(steps, extent[dim] // shards_of).reshape([-1 if axis == dim else 1 for axis in range(len(extent))])
    return level


def distinct(key, rows, count, top, lift):
    ranking = jax.random.permutation(jax.random.fold_in(key, 1), count)
    pull = ranking
    for power in range(3):
        pull = pull * pull // count
    pull = pull * lift // count
    tickets = jax.random.randint(jax.random.fold_in(key, 2), (rows, count), 0, 4096) + pull
    fixed_rows = jax.random.permutation(jax.random.fold_in(key, 3), rows)[jnp.arange(count) % rows]
    tickets = jnp.where(jnp.arange(rows)[:, None] == fixed_rows[None, :], 1 << 14, tickets)
    score = tickets * count + jnp.arange(count)
    return lax.top_k(score.astype(jnp.int32), top)[1].astype(jnp.int32)


def assign_block(key, own, number, rows, amount, top, bound, skew):
    order = jax.random.permutation(key, amount)
    crowded, usual = shares(amount, rows * top, bound, skew, True), shares(amount, rows * top, bound, skew, False)
    places = jnp.arange(amount)

    def named(tallies, offset_by):
        used = int((tallies > 0).sum())
        fixed = max(1, used // 4)
        moved = fixed + (places - fixed + offset_by * (used - fixed)) % max(1, amount - fixed)
        return jnp.zeros((amount,), jnp.int32).at[order[jnp.where(places < fixed, places, moved)]].set(jnp.asarray(tallies, jnp.int32))

    tallies = jnp.where(number % 4 == 0, named(crowded, number // 4), named(usual, number - number // 4 - 1))
    mixed = jax.random.permutation(jax.random.fold_in(own, 3), amount)
    donor, sink = mixed[0:amount // 2 * 2:2], mixed[1:amount // 2 * 2:2]
    room = jnp.minimum(tallies[donor] - 1, bound - tallies[sink]) // 2
    room = jnp.where((donor == order[0]) | (sink == order[0]) | (tallies[sink] == 0), 0, jnp.maximum(room, 0))
    moved = jax.random.randint(jax.random.fold_in(own, 4), (amount // 2,), 0, 1 << 20) % (room + 1)
    tallies = tallies.at[donor].add(-moved).at[sink].add(moved)
    members = jnp.searchsorted(jnp.cumsum(tallies), jnp.arange(rows * top), side="right").astype(jnp.int32)
    grid = members.reshape(top, rows).T
    grid = grid[jax.random.permutation(jax.random.fold_in(own, 1), rows)]
    offset_by = jax.random.randint(jax.random.fold_in(own, 2), (rows, 1), 0, top)
    return jnp.take_along_axis(grid, (jnp.arange(top)[None, :] + offset_by) % top, axis=1)


def shares(count, total, reach, lean, full):
    portions = [(1 << 20) // math.isqrt(rank ** lean) + 1 for rank in range(1, count + 1)]
    largest = reach if full else min(reach, max(-(-total // count), total * portions[0] // sum(portions)))
    least = 1 if total - largest >= count - 1 else 0
    given, surplus = [largest] + [least] * (count - 1), total - largest - least * (count - 1)
    while surplus > 0:
        free = [i for i in range(1, count) if given[i] < largest] or [i for i in range(1, count) if given[i] < reach]
        pool, budget = sum([portions[i] for i in free]), surplus
        for i in free:
            addition = min(reach - given[i], max(1, budget * portions[i] // pool), surplus)
            given[i] = given[i] + addition
            surplus = surplus - addition
    return np.array(given)


def scatter_about(rng, shape, deviation, most, cuts=(), kind=jnp.bfloat16):
    level = shard_levels(rng, shape, cuts, -0.22, 0.18) if cuts else 1.0
    values = jax.random.normal(rng, shape, jnp.float32) * deviation * level
    return jnp.minimum(jnp.maximum(values, -most), most).astype(kind)


def setup_inputs(seed: int = 0) -> dict:
    key_list = jax.random.split(jax.random.key(seed), 11)
    schur = scatter_about(key_list[0], (SUBS, M, M), M ** -0.5, 0.125, ((0, 128), (1, 4)))
    rhs = scatter_about(key_list[1], (SUBS, M, R), 1.0, 6.0, ((0, 128), (1, 4)), jnp.float32)
    start = scatter_about(key_list[2], (SUBS, M, R), 1.0, 6.0, ((0, 128), (1, 4)), jnp.float32)
    project = scatter_about(key_list[3], (SUBS, FACES, MODES * FPTS), FPTS ** -0.5, 0.75, ((0, 128), (1, 4)))
    coarse_basis = scatter_about(key_list[4], (SUBS, NCV, M), (M // NCV) ** -0.5, 0.375, ((0, 128), (2, 4)))
    owner_of_face_keys = jax.random.split(jax.random.fold_in(key_list[5], 1), SUBS * FACES // FACES)
    owner_of_face_turns = jax.random.permutation(jax.random.fold_in(key_list[5], 3), SUBS * FACES // FACES)
    owner_of_face = jax.vmap(lambda own, number: assign_block(jax.random.fold_in(key_list[5], 2), own, number, FACES, NB, 1, CAP, 2))(owner_of_face_keys, owner_of_face_turns).reshape((SUBS, FACES, 1))
    mortar_of_face = place_ends(jax.random.randint(key_list[6], (SUBS, FACES), 0, MORT_OWN), jax.random.fold_in(key_list[6], 1), 0, MORT_OWN - 1).astype(jnp.int32)
    mortar_order = place_ends(jax.random.randint(key_list[7], (SUBS, MORT_OWN), DEG // 2 - 1, DEG), jax.random.fold_in(key_list[7], 1), DEG // 2 - 1, DEG - 1).astype(jnp.int32)
    subdomain_map = jax.random.permutation(key_list[8], SUBS).astype(jnp.int32)
    vertex_ids = distinct(key_list[9], SUBS, NV, NCV, 0)
    return {"schur": schur, "rhs": rhs, "start": start, "project": project, "coarse_basis": coarse_basis, "owner_of_face": owner_of_face, "mortar_of_face": mortar_of_face, "mortar_order": mortar_order, "subdomain_map": subdomain_map, "vertex_ids": vertex_ids}


relax_weight = 0.5
coarse_weight = 0.5


def apply_one(operands):
    matrix, vector = operands
    return jnp.dot(matrix, vector, preferred_element_type=jnp.float32)


def reference(schur, rhs, start, project, coarse_basis, owner_of_face, mortar_of_face, mortar_order, subdomain_map, vertex_ids):
    highest = lax.Precision.HIGHEST
    holder = subdomain_map.astype(jnp.int32)
    offsets = jnp.take(owner_of_face[:, :, 0], holder, axis=0).astype(jnp.int32)
    places = jnp.arange(SUBS, dtype=jnp.int32)[:, None]
    owners = jnp.mod(places + offsets - REACH, SUBS).astype(jnp.int32)
    mortar_local = jnp.take(mortar_of_face, holder, axis=0).astype(jnp.int32)
    corners = jnp.take(vertex_ids, holder, axis=0).reshape(-1).astype(jnp.int32)
    mortar_keys = (owners * MORT_OWN + mortar_local).reshape(-1).astype(jnp.int32)
    all_mortars = SUBS * MORT_OWN
    counts = jax.ops.segment_sum(jnp.ones(mortar_keys.shape, jnp.float32), mortar_keys, num_segments=all_mortars)
    degree = jnp.arange(MODES, dtype=jnp.int32)
    orders = mortar_order.reshape(all_mortars, 1).astype(jnp.int32)
    keep_mask = ((degree[None, :] // DEG <= orders) & (degree[None, :] % DEG <= orders)).astype(jnp.float32)
    tables = project.reshape(SUBS, FACES, MODES, FPTS).astype(jnp.float32)
    coarse_wide = coarse_basis.astype(jnp.float32)
    traces = start
    for repeat in range(ITERS):
        trace_b = traces.astype(jnp.bfloat16)
        product = lax.map(apply_one, (schur, trace_b))
        residual = (product - rhs).astype(jnp.bfloat16)
        face_res = residual.reshape(SUBS, FACES, FPTS, R).astype(jnp.float32)
        coeffs = jnp.einsum('sfmp,sfpr->sfmr', tables, face_res, precision=highest).astype(jnp.bfloat16)
        mortar_sums = jax.ops.segment_sum(coeffs.astype(jnp.float32).reshape(SUBS * FACES, MODES * R), mortar_keys, num_segments=all_mortars)
        averages = mortar_sums / jnp.maximum(counts, 1.0)[:, None]
        averages = (averages.reshape(all_mortars, MODES, R) * keep_mask[:, :, None]).astype(jnp.bfloat16)
        returned = jnp.take(averages, mortar_keys, axis=0).reshape(SUBS, FACES, MODES, R).astype(jnp.float32)
        lifted = jnp.einsum('sfmp,sfmr->sfpr', tables, returned, precision=highest).reshape(SUBS, M, R)
        partial_value = jnp.einsum('svm,smr->svr', coarse_wide, lifted, precision=highest)
        vertex = jax.ops.segment_sum(partial_value.reshape(SUBS * NCV, R), corners, num_segments=NV)
        picked = jnp.take(vertex, corners, axis=0).reshape(SUBS, NCV, R)
        coarse_corr = jnp.einsum('svm,svr->smr', coarse_wide, picked, precision=highest)
        traces = traces - relax_weight * lifted - coarse_weight * coarse_corr
    return traces
```

```python
import functools

import jax
import jax.numpy as jnp
from jax import lax
from jax.experimental import pallas as pl
from jax.experimental.pallas import tpu as pltpu
from jax.sharding import PartitionSpec as P

MORT_OWN = 16
REACH = 2
LINKS = 2 * REACH + 1
CAP = 8
NCV = 8
ITERS = 2
LANES = 128
MESH = pl.DeviceIdType.MESH
HIGHEST = lax.Precision.HIGHEST
F32 = jnp.float32
BF16 = jnp.bfloat16

relax_weight = 0.5
coarse_weight = 0.5


def iota(shape, dim):
    return lax.broadcasted_iota(jnp.int32, shape, dim)


def dot_nn(a, b):
    return lax.dot_general(a, b, (((1,), (0,)), ((), ())), preferred_element_type=F32)


def dot_nt(a, b):
    return lax.dot_general(a, b, (((1,), (1,)), ((), ())), preferred_element_type=F32)


def halves(x):
    high = x.astype(BF16)
    return high, (x - high.astype(F32)).astype(BF16)


def kernel(
    sizes,
    schur,
    rhs,
    start,
    project,
    coarse,
    owner_t,
    mortar_t,
    order_t,
    holder,
    vertex_t,
    out,
    s4,
    st,
    rh,
    tb,
    af,
    pa,
    ca,
    bd,
    sp,
    wm,
    vm,
    fac,
    acc,
    prod,
    sb,
    ar,
    zs,
    orr,
    rs,
    rr,
    ls,
    lr,
    qm,
    psc,
    dm,
    ps,
    pz,
    ks,
    kr,
    pk,
    own_tab,
    mor_tab,
    ord_tab,
    hol_tab,
    ver_tab,
    lsem,
    ag_s,
    ag_r,
    a2a_s,
    a2a_r,
    ex_s,
    ex_r,
    ret_s,
    ret_r,
    p_s,
    p_r,
    k1_s,
    k1_r,
    k2_s,
    k2_r,
    k3_s,
    k3_r,
    fin_s,
    fin_r,
):
    subs, grps, zs_n, yc_n = sizes
    s = lax.axis_index("sub")
    g = lax.axis_index("grp")
    z = s // yc_n
    yc = lax.rem(s, yc_n)
    cols = s4.shape[2]
    quarter = tb.shape[1] // grps
    half = tb.shape[1] // 2

    def sub_at(step):
        return lax.rem(s + step + subs, subs)

    def grp_at(step):
        return lax.rem(g + step, grps)

    def remote(src, dst, send, recv, where):
        return pltpu.make_async_remote_copy(
            src_ref=src,
            dst_ref=dst,
            send_sem=send,
            recv_sem=recv,
            device_id=where,
            device_id_type=MESH,
        )

    loads = [
        pltpu.make_async_copy(start, st, lsem.at[0]),
        pltpu.make_async_copy(owner_t, own_tab, lsem.at[1]),
        pltpu.make_async_copy(mortar_t, mor_tab, lsem.at[2]),
        pltpu.make_async_copy(order_t, ord_tab, lsem.at[3]),
        pltpu.make_async_copy(holder, hol_tab, lsem.at[4]),
        pltpu.make_async_copy(vertex_t, ver_tab, lsem.at[5]),
        pltpu.make_async_copy(project, pa.at[g], lsem.at[6]),
        pltpu.make_async_copy(coarse, ca.at[g], lsem.at[7]),
        pltpu.make_async_copy(rhs, rh, lsem.at[8]),
    ]
    for q in range(grps):
        loads.append(
            pltpu.make_async_copy(
                schur.at[:, pl.ds(q * cols, cols)], s4.at[q], lsem.at[9 + q]
            )
        )
    for load in loads:
        load.start()

    barrier = pltpu.get_barrier_semaphore()
    partners = [{"grp": grp_at(step)} for step in range(1, grps)]
    partners += [{"sub": sub_at(step)} for step in (-2, -1, 1, 2)]
    partners += [{"sub": lax.rem(z + step, zs_n) * yc_n + yc} for step in range(1, zs_n)]
    partners += [{"sub": z * yc_n + lax.rem(yc + step, yc_n)} for step in range(1, yc_n)]
    for where in partners:
        pl.semaphore_signal(barrier, inc=1, device_id=where, device_id_type=MESH)

    ps[...] = jnp.zeros_like(ps)
    loads[0].wait()
    tb[g] = st[...].astype(BF16)
    pl.semaphore_wait(barrier, len(partners))

    left, right = grp_at(grps - 1), grp_at(1)
    across = grp_at(2)
    top, low = pl.ds(0, half), pl.ds(half, half)

    def gather_start(buf, turn):
        to_right, to_left = {"grp": right}, {"grp": left}
        plan = [
            (buf.at[g, top], to_right),
            (buf.at[g, low], to_left),
            (buf.at[g, low], to_right),
            (buf.at[g, top], to_left),
            (buf.at[left, top], to_right),
            (buf.at[right, low], to_left),
        ]
        copies = [
            remote(ref, ref, ag_s.at[turn, i], ag_r.at[turn, i], where)
            for i, (ref, where) in enumerate(plan)
        ]
        for copy in copies[:4]:
            copy.start()
        return copies

    def gather_forward(copies):
        copies[0].wait_recv()
        copies[4].start()
        copies[1].wait_recv()
        copies[5].start()

    gathered = gather_start(tb, 0)

    for load in loads[1:6]:
        load.wait()
    stacked = jnp.concatenate(
        [own_tab[...].astype(F32), mor_tab[...].astype(F32), ver_tab[...].astype(F32)], axis=0
    ).astype(BF16)
    placed = jnp.where(
        iota((subs, subs), 0) == jnp.broadcast_to(hol_tab[...], (subs, subs)), 1.0, 0.0
    ).astype(BF16)
    moved = dot_nn(stacked, placed)
    faces = own_tab.shape[0]
    held_all, mortar_all = moved[:faces], moved[faces : 2 * faces]
    vertex_all = moved[2 * faces :]

    def column(table, index):
        mask = iota(table.shape, 1) == index
        return jnp.sum(jnp.where(mask, table, 0.0), axis=1, keepdims=True)

    square_i, square_j = iota((faces, faces), 0), iota((faces, faces), 1)

    def as_row(col):
        return jnp.sum(jnp.where(square_i == square_j, col, 0.0), axis=0, keepdims=True)

    held_c = column(held_all, s)
    held_r = as_row(held_c)
    rank_r = jnp.sum(
        jnp.where((held_c == held_r) & (square_i < square_j), 1.0, 0.0), axis=0, keepdims=True
    )
    slot_r = held_r * CAP + rank_r
    rows = iota((wm.shape[0], faces), 0)
    face_of = jnp.left_shift(jnp.right_shift(rows, 7), 3) | (rows & 7)
    slot_c = jnp.sum(
        jnp.where(iota(rows.shape, 1) == face_of, slot_r, 0.0), axis=1, keepdims=True
    )
    r_i, c_i = iota(wm.shape, 0), iota(wm.shape, 1)
    same = (jnp.right_shift(r_i, 3) & 15) == (jnp.right_shift(c_i, 3) & 15)
    slot_of = (jnp.left_shift(jnp.right_shift(c_i, 7), 3) | (c_i & 7)).astype(F32)
    wm[...] = jnp.where(same & (slot_c == slot_of), 1.0, 0.0).astype(BF16)

    width = vm.shape[1]
    lane8 = iota((faces, CAP), 1).astype(F32)
    pick8 = iota((LANES, CAP), 1) == (iota((LANES, CAP), 0) & 7)
    v_r, v_c = iota((LANES, width), 0), iota((LANES, width), 1)
    v_same = jnp.right_shift(v_r, 3) == jnp.right_shift(v_c, 4)
    v_key = (v_c & 15).astype(F32)
    counts = jnp.zeros((1, width), F32)
    for link in range(LINKS):
        sender = sub_at(REACH - link)
        hc, mc = column(held_all, sender), column(mortar_all, sender)
        hr = as_row(hc)
        rank_c = jnp.sum(
            jnp.where((hr == hc) & (square_j < square_i), 1.0, 0.0), axis=1, keepdims=True
        )
        key8 = (
            jnp.sum(
                jnp.where((hc == float(link)) & (rank_c == lane8), mc + 1.0, 0.0),
                axis=0,
                keepdims=True,
            )
            - 1.0
        )
        key_c = jnp.sum(jnp.where(pick8, key8, 0.0), axis=1, keepdims=True)
        block = jnp.where(v_same & (key_c == v_key), 1.0, 0.0)
        counts = counts + jnp.sum(block, axis=0, keepdims=True)
        vm[pl.ds(link * LANES, LANES), :] = block.astype(BF16)
    order_c = column(ord_tab[...].astype(F32), s)
    order_r = jnp.sum(
        jnp.where(iota((MORT_OWN, width), 0) == (iota((MORT_OWN, width), 1) & 15), order_c, 0.0),
        axis=0,
        keepdims=True,
    )
    inverse = 1.0 / jnp.maximum(counts, 1.0)
    row_c = iota((1, width), 1)
    for mg in range(4):
        first = (2 * mg + jnp.right_shift(row_c, 7)).astype(F32)
        second = (jnp.right_shift(row_c, 4) & 7).astype(F32)
        keep = (first <= order_r) & (second <= order_r)
        fac[pl.ds(mg, 1), :] = jnp.where(keep, inverse, 0.0)

    vertex_b = vertex_all.astype(BF16)
    d_rows, d_cols = dm.shape
    here = jnp.where(
        iota((d_rows, subs), 1) == z * yc_n + jnp.right_shift(iota((d_rows, subs), 0), 3), 1.0, 0.0
    ).astype(BF16)
    wanted = dot_nt(here, vertex_b)
    wanted = jnp.sum(
        jnp.where(iota((d_rows, NCV), 1) == (iota((d_rows, NCV), 0) & 7), wanted, 0.0),
        axis=1,
        keepdims=True,
    )
    there = jnp.where(
        iota((subs, d_cols), 0) == jnp.right_shift(iota((subs, d_cols), 1), 3) * yc_n + yc, 1.0, 0.0
    ).astype(BF16)
    given = dot_nn(vertex_b, there)
    given = jnp.sum(
        jnp.where(iota((NCV, d_cols), 0) == (iota((NCV, d_cols), 1) & 7), given, 0.0),
        axis=0,
        keepdims=True,
    )
    dm[...] = jnp.where(wanted == given, 1.0, 0.0).astype(BF16)

    lane = iota((CAP, LANES), 1)
    row8 = iota((CAP, 4 * LANES), 0)
    own_face = row8 == jnp.right_shift(iota((CAP, 4 * LANES), 1), 6)

    def build_block(q):
        def step(i, carry):
            pair = pa[q, :, pl.ds(pl.multiple_of(i * LANES, LANES), LANES)].astype(F32)
            turned = pltpu.roll(pair, LANES // 2, 1)
            even = jnp.where(lane < LANES // 2, pair, turned)
            odd = jnp.where(lane < LANES // 2, turned, pair)
            even = jnp.where(own_face, jnp.concatenate([even] * 4, axis=1), 0.0)
            odd = jnp.where(own_face, jnp.concatenate([odd] * 4, axis=1), 0.0)
            both = jnp.concatenate([even, odd], axis=0).astype(BF16)
            bd[q, pl.ds(pl.multiple_of(i * 16, 16), 16), :] = both
            return carry

        lax.fori_loop(0, pa.shape[2] // LANES, step, 0, unroll=4)

    def fold_block(q, s_block):
        wide = dot_nt(s_block, bd[q]).astype(BF16)
        for mg in range(4):
            sp[mg, :, pl.ds(pl.multiple_of(q * LANES, LANES), LANES)] = wide[
                :, mg * LANES : (mg + 1) * LANES
            ]

    def fold_coarse(q):
        basis = dot_nt(ca[q], bd[q])
        high, rest = halves(basis)
        both = jnp.concatenate([high, rest], axis=0)
        for mg in range(4):
            qm[mg, :, pl.ds(pl.multiple_of(q * LANES, LANES), LANES)] = both[
                :, mg * LANES : (mg + 1) * LANES
            ]

    loads[6].wait()
    loads[7].wait()
    build_block(g)
    for load in loads[8:]:
        load.wait()
    gather_forward(gathered)

    def add_block(q):
        acc[...] += dot_nt(tb[q], s4[q])

    acc[...] = dot_nt(tb[g], s4[g])
    gathered[2].wait_recv()
    add_block(left)
    gathered[3].wait_recv()
    add_block(right)
    gathered[4].wait_recv()
    gathered[5].wait_recv()
    add_block(across)
    prod[...] = acc[...] - rh[...]

    extra = []
    sent = list(gathered)

    def exchange(turn, residual, picked):
        coeffs = dot_nt(residual.astype(BF16), bd[g]).astype(BF16)
        for q in range(grps):
            for mg in range(4):
                sb[turn, q, pl.ds(mg * quarter, quarter), :] = coeffs[
                    q * quarter : (q + 1) * quarter, mg * LANES : (mg + 1) * LANES
                ]
        swaps = []
        for i in range(grps - 1):
            to = grp_at(i + 1)
            swap = remote(
                sb.at[turn, to], ar.at[turn, g], a2a_s.at[turn, i], a2a_r.at[turn, i], {"grp": to}
            )
            swap.start()
            swaps.append(swap)
        ar[turn, g] = sb[turn, g]
        if turn == 0:
            for i in range(grps - 1):
                to = grp_at(i + 1)
                extra.append(remote(ca.at[g], ca.at[g], p_s.at[0, i], p_r.at[0, i], {"grp": to}))
                extra.append(remote(pa.at[g], pa.at[g], p_s.at[1, i], p_r.at[1, i], {"grp": to}))
            for copy in extra:
                copy.start()
            fold_block(g, s4[g])
            fold_coarse(g)
        for swap in swaps:
            swap.wait_recv()
        lines = [ar[turn, q] for q in range(grps)]
        if picked is not None:
            narrow = picked()
            for q in range(grps):
                term = jnp.dot(
                    narrow, psc[q], preferred_element_type=F32, precision=HIGHEST
                )
                tall = jnp.concatenate(
                    [term[:, mg * LANES : (mg + 1) * LANES] for mg in range(4)], axis=0
                )
                lines[q] = (lines[q].astype(F32) - coarse_weight * tall).astype(BF16)
        grouped = dot_nn(jnp.concatenate(lines, axis=1), wm[...]).astype(BF16)
        sends = []
        for link in (0, 4, 1, 3, 2):
            part = grouped[:, link * LANES : (link + 1) * LANES]
            if link == REACH:
                orr[turn, link] = part
                continue
            zs[turn, link] = part
            copy = remote(
                zs.at[turn, link],
                orr.at[turn, link],
                ex_s.at[turn, link],
                ex_r.at[turn, link],
                {"sub": sub_at(link - REACH)},
            )
            copy.start()
            sends.append(copy)
        if turn == 0:
            for copy in extra:
                copy.wait_recv()
            for i in range(grps - 1):
                build_block(grp_at(i + 1))
        for copy in sends:
            copy.wait_recv()
        joined = jnp.concatenate([orr[turn, link] for link in range(LINKS)], axis=1)
        sums = dot_nn(joined, vm[...])
        averages = jnp.concatenate(
            [
                sums[mg * quarter : (mg + 1) * quarter] * fac[pl.ds(mg, 1), :]
                for mg in range(4)
            ],
            axis=0,
        ).astype(BF16)
        replies = dot_nt(averages, vm[...]).astype(BF16)
        backs = []
        for link in (0, 4, 1, 3, 2):
            part = replies[:, link * LANES : (link + 1) * LANES]
            if link == REACH:
                rr[turn, link] = part
                continue
            rs[turn, link] = part
            copy = remote(
                rs.at[turn, link],
                rr.at[turn, link],
                ret_s.at[turn, link],
                ret_r.at[turn, link],
                {"sub": sub_at(REACH - link)},
            )
            copy.start()
            backs.append(copy)
        if turn == 0:
            for i in range(grps - 1):
                q = grp_at(i + 1)
                fold_block(q, s4[q])
                fold_coarse(q)
            spread = dot_nt(ca[0], s4[0])
            for q in range(1, grps):
                spread = spread + dot_nt(ca[q], s4[q])
            high, rest = halves(spread)
            psc[g] = dot_nt(high, bd[g]) + dot_nt(rest, bd[g])
            for i in range(grps - 1):
                to = grp_at(i + 1)
                copy = remote(psc.at[g], psc.at[g], p_s.at[2, i], p_r.at[2, i], {"grp": to})
                copy.start()
                extra.append(copy)
        for copy in backs:
            copy.wait_recv()
        sent.extend(swaps + sends + backs)
        answered = jnp.concatenate([rr[turn, link] for link in range(LINKS)], axis=1)
        return dot_nt(answered, wm[...]).astype(BF16)

    def coarse_first(turn, mine):
        value = dot_nt(qm[0], mine[:quarter])
        for mg in range(1, 4):
            value = value + dot_nt(qm[mg], mine[mg * quarter : (mg + 1) * quarter])
        ps[turn, :, pl.ds(0, quarter)] = value[:NCV] + value[NCV:]
        copies = []
        for i in range(zs_n - 1):
            to = lax.rem(z + i + 1, zs_n) * yc_n + yc
            copy = remote(
                ps.at[turn], pz.at[turn, z], k1_s.at[turn, i], k1_r.at[turn, i], {"sub": to}
            )
            copy.start()
            copies.append(copy)
        pz[turn, z] = ps[turn]
        sent.extend(copies)
        return copies

    def coarse_second(turn, copies):
        for copy in copies:
            copy.wait_recv()
        high, rest = halves(pz[turn].reshape(zs_n * NCV, LANES))
        value = dot_nn(dm[...], high) + dot_nn(dm[...], rest)
        ks[turn] = value.reshape(yc_n, NCV, LANES)
        copies = []
        for i in range(yc_n - 1):
            to = lax.rem(yc + i + 1, yc_n)
            copy = remote(
                ks.at[turn, to],
                kr.at[turn, yc],
                k2_s.at[turn, i],
                k2_r.at[turn, i],
                {"sub": z * yc_n + to},
            )
            copy.start()
            copies.append(copy)
        kr[turn, yc] = ks[turn, yc]
        sent.extend(copies)
        return copies

    mine = exchange(0, prod[...], None)
    af[g] = mine
    gathered = gather_start(af, 1)
    sent.extend(gathered)
    first_copies = coarse_first(0, mine)

    def add_modes(q):
        value = dot_nt(af[q, pl.ds(0, quarter), :], sp[0])
        for mg in range(1, 4):
            value = value + dot_nt(af[q, pl.ds(mg * quarter, quarter), :], sp[mg])
        at = pl.ds(pl.multiple_of(q * quarter, quarter), quarter)
        acc[at, :] = prod[at, :] - relax_weight * value

    add_modes(g)
    gather_forward(gathered)
    gathered[2].wait_recv()
    add_modes(left)
    gathered[3].wait_recv()
    add_modes(right)
    second_copies = coarse_second(0, first_copies)
    gathered[4].wait_recv()
    gathered[5].wait_recv()
    add_modes(across)
    for copy in extra[2 * (grps - 1) :]:
        copy.wait_recv()
    totals = []

    def first_picked():
        for copy in second_copies:
            copy.wait_recv()
        picked = jnp.sum(kr[0], axis=0)
        totals.append(picked)
        return picked.T[:quarter]

    mine = exchange(1, acc[...], first_picked)
    first_copies = coarse_first(1, mine)
    backs = []
    for q in range(grps):
        ls[q] = mine[:, q * LANES : (q + 1) * LANES]
    for i in range(grps - 1):
        to = grp_at(i + 1)
        copy = remote(ls.at[to], lr.at[g], fin_s.at[i], fin_r.at[i], {"grp": to})
        copy.start()
        backs.append(copy)
    lr[g] = ls[g]

    def own_rows(blocks):
        lines = [
            jnp.concatenate(
                [block[mg * quarter : (mg + 1) * quarter] for mg in range(4)], axis=1
            )
            for block in blocks
        ]
        return jnp.concatenate(lines, axis=0)

    here = pl.ds(pl.multiple_of(g * LANES, LANES), LANES)
    lifted = dot_nn(own_rows([af[q, :, here] for q in range(grps)]), bd[g])
    for copy in backs:
        copy.wait_recv()
    lifted = lifted + dot_nn(own_rows([lr[q] for q in range(grps)]), bd[g])
    acc[...] = st[...] - relax_weight * lifted

    second_copies = coarse_second(1, first_copies)
    for copy in second_copies:
        copy.wait_recv()
    pk[g] = jnp.sum(kr[1], axis=0) + totals[0]
    last = []
    for i in range(grps - 1):
        to = grp_at(i + 1)
        copy = remote(pk.at[g], pk.at[g], k3_s.at[i], k3_r.at[i], {"grp": to})
        copy.start()
        last.append(copy)
    for copy in last:
        copy.wait_recv()
    tall = jnp.concatenate([pk[q].T[:quarter] for q in range(grps)], axis=0)
    corr = jnp.dot(
        tall, ca[g].astype(F32), preferred_element_type=F32, precision=HIGHEST
    )
    out[...] = acc[...] - coarse_weight * corr
    for copy in sent + extra + backs + last:
        copy.wait_send()


def solution(mesh):
    subs, grps = mesh.shape["sub"], mesh.shape["grp"]
    zs_n = 8 if subs == 128 else 2
    yc_n = subs // zs_n
    sizes = (subs, grps, zs_n, yc_n)

    def body(
        schur,
        rhs,
        start,
        project,
        coarse_basis,
        owner_of_face,
        mortar_of_face,
        mortar_order,
        subdomain_map,
        vertex_ids,
    ):
        rows, cols = schur.shape[1], schur.shape[2]
        part = cols // grps
        wide = rhs.shape[2]
        faces = owner_of_face.shape[1]
        block = LANES
        dma = pltpu.SemaphoreType.DMA
        vmem = pltpu.VMEM
        scratch = [
            vmem((grps, rows, part), BF16),
            vmem((wide, rows), F32),
            vmem((wide, rows), F32),
            vmem((grps, wide, rows), BF16),
            vmem((grps, wide, rows), BF16),
            vmem((grps,) + project.shape[1:], BF16),
            vmem((grps,) + coarse_basis.shape[1:], BF16),
            vmem((grps, rows, rows), BF16),
            vmem((4, rows, rows), BF16),
            vmem((rows, LINKS * block), BF16),
            vmem((LINKS * block, 16 * MORT_OWN), BF16),
            vmem((8, 16 * MORT_OWN), F32),
            vmem((wide, rows), F32),
            vmem((wide, rows), F32),
            vmem((ITERS, grps, wide, block), BF16),
            vmem((ITERS, grps, wide, block), BF16),
            vmem((ITERS, LINKS, wide, block), BF16),
            vmem((ITERS, LINKS, wide, block), BF16),
            vmem((ITERS, LINKS, wide, block), BF16),
            vmem((ITERS, LINKS, wide, block), BF16),
            vmem((grps, wide, block), BF16),
            vmem((grps, wide, block), BF16),
            vmem((4, 2 * NCV, rows), BF16),
            vmem((grps, NCV, rows), F32),
            vmem((yc_n * NCV, zs_n * NCV), BF16),
            vmem((ITERS, NCV, LANES), F32),
            vmem((ITERS, zs_n, NCV, LANES), F32),
            vmem((ITERS, yc_n, NCV, LANES), F32),
            vmem((ITERS, yc_n, NCV, LANES), F32),
            vmem((grps, NCV, LANES), F32),
            vmem((faces, subs), jnp.int32),
            vmem((faces, subs), jnp.int32),
            vmem((MORT_OWN, subs), jnp.int32),
            vmem((1, subs), jnp.int32),
            vmem((NCV, subs), jnp.int32),
            dma((9 + grps,)),
            dma((2, 6)),
            dma((2, 6)),
            dma((ITERS, grps - 1)),
            dma((ITERS, grps - 1)),
            dma((ITERS, LINKS)),
            dma((ITERS, LINKS)),
            dma((ITERS, LINKS)),
            dma((ITERS, LINKS)),
            dma((3, grps - 1)),
            dma((3, grps - 1)),
            dma((ITERS, zs_n - 1)),
            dma((ITERS, zs_n - 1)),
            dma((ITERS, yc_n - 1)),
            dma((ITERS, yc_n - 1)),
            dma((grps - 1,)),
            dma((grps - 1,)),
            dma((grps - 1,)),
            dma((grps - 1,)),
        ]
        result = pl.pallas_call(
            functools.partial(kernel, sizes),
            out_shape=jax.ShapeDtypeStruct((wide, rows), F32),
            in_specs=[pl.BlockSpec(memory_space=pltpu.HBM)] * 10,
            out_specs=pl.BlockSpec(memory_space=pltpu.VMEM),
            scratch_shapes=scratch,
            compiler_params=pltpu.CompilerParams(
                collective_id=0, has_side_effects=True, vmem_limit_bytes=66 * 1000 * 1000
            ),
        )(
            schur[0],
            rhs[0].T,
            start[0].T,
            project[0],
            coarse_basis[0],
            owner_of_face[:, :, 0].T,
            mortar_of_face.T,
            mortar_order.T,
            subdomain_map.reshape(1, subs),
            vertex_ids.T,
        )
        return result.T[None]

    split = P("sub", "grp", None)
    return jax.shard_map(
        body,
        mesh=mesh,
        in_specs=(split, split, split, split, P("sub", None, "grp"), P(), P(), P(), P(), P()),
        out_specs=split,
        check_vma=False,
    )
```

```python
import functools

import jax
import jax.numpy as jnp
from jax import lax
from jax.experimental import pallas as pl
from jax.experimental.pallas import tpu as pltpu
from jax.sharding import PartitionSpec as P

MORT_OWN = 16
REACH = 2
LINKS = 2 * REACH + 1
CAP = 8
NCV = 8
ITERS = 2
PARTS = 2
LANES = 128
MESH = pl.DeviceIdType.MESH
HIGHEST = lax.Precision.HIGHEST
F32 = jnp.float32
BF16 = jnp.bfloat16

relax_weight = 0.5
coarse_weight = 0.5


def iota(shape, dim):
    return lax.broadcasted_iota(jnp.int32, shape, dim)


def dot_nn(a, b):
    return lax.dot_general(a, b, (((1,), (0,)), ((), ())), preferred_element_type=F32)


def dot_nt(a, b):
    return lax.dot_general(a, b, (((1,), (1,)), ((), ())), preferred_element_type=F32)


def halves(x):
    high = x.astype(BF16)
    return high, (x - high.astype(F32)).astype(BF16)


def kernel(
    sizes,
    schur,
    rhs,
    start,
    project,
    coarse,
    owner_t,
    mortar_t,
    order_t,
    holder,
    vertex_t,
    out,
    s4,
    st,
    rh,
    tb,
    af,
    pa,
    ca,
    bd,
    sp,
    wm,
    vm,
    fac,
    acc,
    prod,
    sb,
    ar,
    zs,
    orr,
    rs,
    rr,
    ls,
    lr,
    qm,
    psc,
    dm,
    ps,
    pz,
    ks,
    kr,
    pk,
    own_tab,
    mor_tab,
    ord_tab,
    hol_tab,
    ver_tab,
    lsem,
    ag_s,
    ag_r,
    a2a_s,
    a2a_r,
    ex_s,
    ex_r,
    ret_s,
    ret_r,
    p_s,
    p_r,
    k1_s,
    k1_r,
    k2_s,
    k2_r,
    k3_s,
    k3_r,
    fin_s,
    fin_r,
):
    subs, grps, zs_n, yc_n = sizes
    s = lax.axis_index("sub")
    g = lax.axis_index("grp")
    z = s // yc_n
    yc = lax.rem(s, yc_n)
    cols = s4.shape[2]
    quarter = tb.shape[1] // grps
    half = tb.shape[1] // 2

    def sub_at(step):
        return lax.rem(s + step + subs, subs)

    def grp_at(step):
        return lax.rem(g + step, grps)

    def remote(src, dst, send, recv, where):
        return pltpu.make_async_remote_copy(
            src_ref=src,
            dst_ref=dst,
            send_sem=send,
            recv_sem=recv,
            device_id=where,
            device_id_type=MESH,
        )

    def whole(ref, sem):
        return remote(ref, ref, sem, sem, {"grp": grp_at(1)})

    def arrive(name, *parts):
        with jax.named_scope(name):
            for ref, sem in parts:
                whole(ref, sem).wait_recv()

    barrier = pltpu.get_barrier_semaphore()
    partners = [{"sub": lax.rem(z + step, zs_n) * yc_n + yc} for step in range(1, zs_n)]
    partners += [{"sub": z * yc_n + lax.rem(yc + step, yc_n)} for step in range(1, yc_n)]
    partners += [{"sub": sub_at(step)} for step in (-2, -1, 1, 2)]
    partners += [{"grp": grp_at(step)} for step in range(1, grps)]
    for where in partners:
        pl.semaphore_signal(barrier, inc=1, device_id=where, device_id_type=MESH)

    loads = [
        pltpu.make_async_copy(start, st, lsem.at[0]),
        pltpu.make_async_copy(owner_t, own_tab, lsem.at[1]),
        pltpu.make_async_copy(mortar_t, mor_tab, lsem.at[2]),
        pltpu.make_async_copy(order_t, ord_tab, lsem.at[3]),
        pltpu.make_async_copy(holder, hol_tab, lsem.at[4]),
        pltpu.make_async_copy(vertex_t, ver_tab, lsem.at[5]),
        pltpu.make_async_copy(project, pa.at[g], lsem.at[6]),
        pltpu.make_async_copy(coarse, ca.at[g], lsem.at[7]),
        pltpu.make_async_copy(rhs, rh, lsem.at[8]),
    ]
    for q in range(grps):
        loads.append(
            pltpu.make_async_copy(
                schur.at[:, pl.ds(q * cols, cols)], s4.at[q], lsem.at[9 + q]
            )
        )
    for load in loads:
        load.start()

    with jax.named_scope("w_start"):
        loads[0].wait()
    tb[g] = st[...].astype(BF16)
    with jax.named_scope("w_barrier"):
        pl.semaphore_wait(barrier, len(partners))

    left, right = grp_at(grps - 1), grp_at(1)
    across = grp_at(2)
    to_right, to_left = {"grp": right}, {"grp": left}

    def gather_plan(buf, turn):
        def piece(q, i):
            return buf.at[q, pl.ds(i * quarter, quarter)]

        def send(q, i, place, where):
            ref = piece(q, i)
            remote(ref, ref, ag_s.at[turn], ag_r.at[turn, place], where).start()

        far = [2 * grps + turn * (i // 2) for i in range(grps)]
        return piece, send, far

    def gather_send(plan, i):
        _, send, _ = plan
        send(g, i, i, to_right)
        send(g, i + 1, grps + i + 1, to_left)
        send(g, i + 1, i + 1, to_right)
        send(g, i, grps + i, to_left)

    def from_left(plan, turn, i):
        return plan[0](left, i), ag_r.at[turn, i]

    def from_right(plan, turn, i):
        return plan[0](right, i), ag_r.at[turn, grps + i]

    def gather_forward(plan, turn, i):
        _, send, far = plan
        if i % 2:
            arrive("w_near", from_right(plan, turn, i))
            send(right, i, far[i], to_left)
        else:
            arrive("w_near", from_left(plan, turn, i))
            send(left, i, far[i], to_right)

    gathered = gather_plan(tb, 0)
    for i in range(0, grps, 2):
        gather_send(gathered, i)

    ps[...] = jnp.zeros_like(ps)
    for load in loads[1:6]:
        load.wait()
    stacked = jnp.concatenate(
        [own_tab[...].astype(F32), mor_tab[...].astype(F32), ver_tab[...].astype(F32)], axis=0
    ).astype(BF16)
    placed = jnp.where(
        iota((subs, subs), 0) == jnp.broadcast_to(hol_tab[...], (subs, subs)), 1.0, 0.0
    ).astype(BF16)
    moved = dot_nn(stacked, placed)
    faces = own_tab.shape[0]
    held_all, mortar_all = moved[:faces], moved[faces : 2 * faces]
    vertex_all = moved[2 * faces :]

    def column(table, index):
        mask = iota(table.shape, 1) == index
        return jnp.sum(jnp.where(mask, table, 0.0), axis=1, keepdims=True)

    square_i, square_j = iota((faces, faces), 0), iota((faces, faces), 1)

    def as_row(col):
        return jnp.sum(jnp.where(square_i == square_j, col, 0.0), axis=0, keepdims=True)

    held_c = column(held_all, s)
    held_r = as_row(held_c)
    rank_r = jnp.sum(
        jnp.where((held_c == held_r) & (square_i < square_j), 1.0, 0.0), axis=0, keepdims=True
    )
    slot_r = held_r * CAP + rank_r
    rows = iota((wm.shape[0], faces), 0)
    face_of = jnp.left_shift(jnp.right_shift(rows, 7), 3) | (rows & 7)
    slot_c = jnp.sum(
        jnp.where(iota(rows.shape, 1) == face_of, slot_r, 0.0), axis=1, keepdims=True
    )
    r_i, c_i = iota(wm.shape, 0), iota(wm.shape, 1)
    same = (jnp.right_shift(r_i, 3) & 15) == (jnp.right_shift(c_i, 3) & 15)
    slot_of = (jnp.left_shift(jnp.right_shift(c_i, 7), 3) | (c_i & 7)).astype(F32)
    wm[...] = jnp.where(same & (slot_c == slot_of), 1.0, 0.0).astype(BF16)

    width = vm.shape[1]
    lane8 = iota((faces, CAP), 1).astype(F32)
    pick8 = iota((LANES, CAP), 1) == (iota((LANES, CAP), 0) & 7)
    v_r, v_c = iota((LANES, width), 0), iota((LANES, width), 1)
    v_same = jnp.right_shift(v_r, 3) == jnp.right_shift(v_c, 4)
    v_key = (v_c & 15).astype(F32)
    counts = jnp.zeros((1, width), F32)
    for link in range(LINKS):
        sender = sub_at(REACH - link)
        hc, mc = column(held_all, sender), column(mortar_all, sender)
        hr = as_row(hc)
        rank_c = jnp.sum(
            jnp.where((hr == hc) & (square_j < square_i), 1.0, 0.0), axis=1, keepdims=True
        )
        key8 = (
            jnp.sum(
                jnp.where((hc == float(link)) & (rank_c == lane8), mc + 1.0, 0.0),
                axis=0,
                keepdims=True,
            )
            - 1.0
        )
        key_c = jnp.sum(jnp.where(pick8, key8, 0.0), axis=1, keepdims=True)
        block = jnp.where(v_same & (key_c == v_key), 1.0, 0.0)
        counts = counts + jnp.sum(block, axis=0, keepdims=True)
        vm[pl.ds(link * LANES, LANES), :] = block.astype(BF16)
    order_c = column(ord_tab[...].astype(F32), s)
    order_r = jnp.sum(
        jnp.where(iota((MORT_OWN, width), 0) == (iota((MORT_OWN, width), 1) & 15), order_c, 0.0),
        axis=0,
        keepdims=True,
    )
    inverse = 1.0 / jnp.maximum(counts, 1.0)
    row_c = iota((1, width), 1)
    for mg in range(4):
        first = (2 * mg + jnp.right_shift(row_c, 7)).astype(F32)
        second = (jnp.right_shift(row_c, 4) & 7).astype(F32)
        keep = (first <= order_r) & (second <= order_r)
        fac[pl.ds(mg, 1), :] = jnp.where(keep, inverse, 0.0)

    vertex_b = vertex_all.astype(BF16)
    d_rows, d_cols = dm.shape
    here = jnp.where(
        iota((d_rows, subs), 1) == z * yc_n + jnp.right_shift(iota((d_rows, subs), 0), 3), 1.0, 0.0
    ).astype(BF16)
    wanted = dot_nt(here, vertex_b)
    wanted = jnp.sum(
        jnp.where(iota((d_rows, NCV), 1) == (iota((d_rows, NCV), 0) & 7), wanted, 0.0),
        axis=1,
        keepdims=True,
    )
    there = jnp.where(
        iota((subs, d_cols), 0) == jnp.right_shift(iota((subs, d_cols), 1), 3) * yc_n + yc, 1.0, 0.0
    ).astype(BF16)
    given = dot_nn(vertex_b, there)
    given = jnp.sum(
        jnp.where(iota((NCV, d_cols), 0) == (iota((NCV, d_cols), 1) & 7), given, 0.0),
        axis=0,
        keepdims=True,
    )
    dm[...] = jnp.where(wanted == given, 1.0, 0.0).astype(BF16)

    lane = iota((CAP, LANES), 1)
    row8 = iota((CAP, 4 * LANES), 0)
    own_face = row8 == jnp.right_shift(iota((CAP, 4 * LANES), 1), 6)

    def build_block(q):
        def step(i, carry):
            pair = pa[q, :, pl.ds(pl.multiple_of(i * LANES, LANES), LANES)].astype(F32)
            turned = pltpu.roll(pair, LANES // 2, 1)
            even = jnp.where(lane < LANES // 2, pair, turned)
            odd = jnp.where(lane < LANES // 2, turned, pair)
            even = jnp.where(own_face, jnp.concatenate([even] * 4, axis=1), 0.0)
            odd = jnp.where(own_face, jnp.concatenate([odd] * 4, axis=1), 0.0)
            both = jnp.concatenate([even, odd], axis=0).astype(BF16)
            bd[q, pl.ds(pl.multiple_of(i * 16, 16), 16), :] = both
            return carry

        lax.fori_loop(0, pa.shape[2] // LANES, step, 0, unroll=4)

    def fold_block(q, s_block):
        wide = dot_nt(s_block, bd[q]).astype(BF16)
        for mg in range(4):
            sp[mg, :, pl.ds(pl.multiple_of(q * LANES, LANES), LANES)] = wide[
                :, mg * LANES : (mg + 1) * LANES
            ]

    def fold_coarse(q):
        both = jnp.concatenate(halves(dot_nt(ca[q], bd[q])), axis=0)
        for mg in range(4):
            qm[mg, :, pl.ds(pl.multiple_of(q * LANES, LANES), LANES)] = both[
                :, mg * LANES : (mg + 1) * LANES
            ]

    loads[6].wait()
    loads[7].wait()
    with jax.named_scope("c_block"):
        build_block(g)
    with jax.named_scope("w_loads"):
        for load in loads[8:]:
            load.wait()
    for i in range(grps):
        gather_forward(gathered, 0, i)

    def add_block(q):
        acc[...] += dot_nt(tb[q], s4[q])

    acc[...] = dot_nt(tb[g], s4[g])
    arrive("w_left", from_left(gathered, 0, 1), from_left(gathered, 0, 3))
    add_block(left)
    arrive("w_right", from_right(gathered, 0, 0), from_right(gathered, 0, 2))
    add_block(right)
    arrive("w_across", (tb.at[across], ag_r.at[0, 2 * grps]))
    add_block(across)
    prod[...] = acc[...] - rh[...]

    groups = 4 // PARTS
    span = groups * quarter

    def rows_of(part):
        return pl.ds(part * span, span)

    def exchange(turn, residual, picked, deliver):
        residual = residual.astype(BF16)
        for part in range(PARTS):
            first = part * groups
            modes = bd[g, pl.ds(first * LANES, groups * LANES), :]
            coeffs = dot_nt(residual, modes).astype(BF16)
            for q in range(grps):
                for mg in range(groups):
                    sb[turn, q, pl.ds((first + mg) * quarter, quarter), :] = coeffs[
                        q * quarter : (q + 1) * quarter, mg * LANES : (mg + 1) * LANES
                    ]
            for i in (2, 1, 3):
                to = grp_at(i)
                remote(
                    sb.at[turn, to, rows_of(part)],
                    ar.at[turn, g, rows_of(part)],
                    a2a_s.at[turn],
                    a2a_r.at[turn, part],
                    {"grp": to},
                ).start()
        ar[turn, g] = sb[turn, g]
        if turn == 0:
            for i, ref in enumerate((ca, pa)):
                for step in (2, 1, 3):
                    where = {"grp": grp_at(step)}
                    remote(ref.at[g], ref.at[g], p_s.at[i], p_r.at[i], where).start()
            fold_block(g, s4[g])
            fold_coarse(g)
        terms = None if picked is None else picked()
        for part in range(PARTS):
            arrive("w_a2a", (ar.at[turn, pl.ds(0, grps - 1), rows_of(part)], a2a_r.at[turn, part]))
            lines = [ar[turn, q, rows_of(part), :] for q in range(grps)]
            if terms is not None:
                for q in range(grps):
                    tall = jnp.concatenate(
                        [
                            terms[q][:, mg * LANES : (mg + 1) * LANES]
                            for mg in range(part * groups, (part + 1) * groups)
                        ],
                        axis=0,
                    )
                    lines[q] = (lines[q].astype(F32) - coarse_weight * tall).astype(BF16)
            grouped = dot_nn(jnp.concatenate(lines, axis=1), wm[...]).astype(BF16)
            for link in (0, 4, 1, 3, 2):
                piece = grouped[:, link * LANES : (link + 1) * LANES]
                if link == REACH:
                    orr[turn, link, rows_of(part), :] = piece
                    continue
                zs[turn, link, rows_of(part), :] = piece
                remote(
                    zs.at[turn, link, rows_of(part)],
                    orr.at[turn, link, rows_of(part)],
                    ex_s.at[turn],
                    ex_r.at[turn, part],
                    {"sub": sub_at(link - REACH)},
                ).start()
        if turn == 0:
            others = pl.ds(0, grps - 1)
            arrive("w_extra", (ca.at[others], p_r.at[0]), (pa.at[others], p_r.at[1]))
            for i in range(grps - 1):
                build_block(grp_at(i + 1))
        for part in range(PARTS):
            arrive("w_ex", (orr.at[turn, pl.ds(0, LINKS - 1), rows_of(part)], ex_r.at[turn, part]))
            joined = jnp.concatenate(
                [orr[turn, link, rows_of(part), :] for link in range(LINKS)], axis=1
            )
            sums = dot_nn(joined, vm[...])
            averages = jnp.concatenate(
                [
                    sums[mg * quarter : (mg + 1) * quarter]
                    * fac[pl.ds(part * groups + mg, 1), :]
                    for mg in range(groups)
                ],
                axis=0,
            ).astype(BF16)
            replies = dot_nt(averages, vm[...]).astype(BF16)
            for link in (0, 4, 1, 3, 2):
                piece = replies[:, link * LANES : (link + 1) * LANES]
                if link == REACH:
                    rr[turn, link, rows_of(part), :] = piece
                    continue
                rs[turn, link, rows_of(part), :] = piece
                remote(
                    rs.at[turn, link, rows_of(part)],
                    rr.at[turn, link, rows_of(part)],
                    ret_s.at[turn],
                    ret_r.at[turn, part],
                    {"sub": sub_at(REACH - link)},
                ).start()
        if turn == 0:
            for i in range(grps - 1):
                q = grp_at(i + 1)
                fold_block(q, s4[q])
                fold_coarse(q)
            spread = dot_nt(ca[0], s4[0])
            for q in range(1, grps):
                spread = spread + dot_nt(ca[q], s4[q])
            high, rest = halves(spread)
            psc[g] = jnp.concatenate(
                halves(dot_nt(high, bd[g]) + dot_nt(rest, bd[g])), axis=0
            )
            for step in (2, 1, 3):
                where = {"grp": grp_at(step)}
                remote(psc.at[g], psc.at[g], p_s.at[2], p_r.at[2], where).start()
        for part in range(PARTS):
            arrive("w_ret", (rr.at[turn, pl.ds(0, LINKS - 1), rows_of(part)], ret_r.at[turn, part]))
            answered = jnp.concatenate(
                [rr[turn, link, rows_of(part), :] for link in range(LINKS)], axis=1
            )
            deliver(part, dot_nt(answered, wm[...]).astype(BF16))

    def coarse_part(part, mine):
        value = dot_nt(qm[part * groups], mine[:quarter])
        for mg in range(1, groups):
            value = value + dot_nt(
                qm[part * groups + mg], mine[mg * quarter : (mg + 1) * quarter]
            )
        return value[:NCV] + value[NCV:]

    def coarse_first(turn, value):
        ps[turn, :, pl.ds(0, quarter)] = value
        for step in range(zs_n - 1):
            to = lax.rem(z + step + 1, zs_n) * yc_n + yc
            remote(
                ps.at[turn], pz.at[turn, z], k1_s.at[turn], k1_r.at[turn], {"sub": to}
            ).start()
        pz[turn, z] = ps[turn]

    def coarse_second(turn):
        arrive("w_k1", (pz.at[turn, pl.ds(0, zs_n - 1)], k1_r.at[turn]))
        high, rest = halves(pz[turn].reshape(zs_n * NCV, LANES))
        value = dot_nn(dm[...], high) + dot_nn(dm[...], rest)
        ks[turn] = value.reshape(yc_n, NCV, LANES)
        for step in range(yc_n - 1):
            to = lax.rem(yc + step + 1, yc_n)
            remote(
                ks.at[turn, to],
                kr.at[turn, yc],
                k2_s.at[turn],
                k2_r.at[turn],
                {"sub": z * yc_n + to},
            ).start()
        kr[turn, yc] = ks[turn, yc]

    def coarse_third(turn):
        arrive("w_k2", (kr.at[turn, pl.ds(0, yc_n - 1)], k2_r.at[turn]))
        return jnp.sum(kr[turn], axis=0)

    gathered = gather_plan(af, 1)
    sums = []

    def spread_out(part, mine):
        af[g, rows_of(part), :] = mine
        for i in range(part * groups, (part + 1) * groups, 2):
            gather_send(gathered, i)
        sums.append(coarse_part(part, mine))
        if part == PARTS - 1:
            coarse_first(0, sum(sums))

    exchange(0, prod[...], None, spread_out)

    def add_modes(q, groups_of, fresh):
        at = pl.ds(pl.multiple_of(q * quarter, quarter), quarter)
        value = dot_nt(af[q, pl.ds(groups_of[0] * quarter, quarter), :], sp[groups_of[0]])
        for mg in groups_of[1:]:
            value = value + dot_nt(af[q, pl.ds(mg * quarter, quarter), :], sp[mg])
        base = prod if fresh else acc
        acc[at, :] = base[at, :] - relax_weight * value

    add_modes(g, (0, 1, 2, 3), True)
    gather_forward(gathered, 1, 0)
    gather_forward(gathered, 1, 1)
    arrive("w_left", from_left(gathered, 1, 1))
    add_modes(left, (0, 1), True)
    arrive("w_right", from_right(gathered, 1, 0))
    add_modes(right, (0, 1), True)
    gather_forward(gathered, 1, 2)
    gather_forward(gathered, 1, 3)
    coarse_second(0)
    arrive("w_left", from_left(gathered, 1, 3))
    add_modes(left, (2, 3), False)
    arrive("w_right", from_right(gathered, 1, 2))
    add_modes(right, (2, 3), False)
    for part in range(2):
        far = af.at[across, pl.ds(2 * part * quarter, 2 * quarter)]
        arrive("w_across", (far, ag_r.at[1, 2 * grps + part]))
        add_modes(across, (2 * part, 2 * part + 1), part == 0)
    totals = []

    def first_picked():
        arrive("w_psc", (psc.at[pl.ds(0, grps - 1)], p_r.at[2]))
        picked = coarse_third(0)
        totals.append(picked)
        high, rest = halves(picked.T[:quarter])
        both = jnp.concatenate(
            [jnp.concatenate([high, high], axis=1), jnp.concatenate([rest, rest], axis=1)],
            axis=0,
        )
        terms = []
        for q in range(grps):
            term = dot_nn(both, psc[q])
            terms.append(term[:quarter] + term[quarter:])
        return terms

    final_sums = []

    def hand_back(part, mine):
        final_sums.append(coarse_part(part, mine))
        if part == PARTS - 1:
            coarse_first(1, sum(final_sums))
        for q in range(grps):
            ls[q, rows_of(part), :] = mine[:, q * LANES : (q + 1) * LANES]
        for step in (2, 1, 3):
            to = grp_at(step)
            remote(
                ls.at[to, rows_of(part)], lr.at[g, rows_of(part)], fin_s, fin_r, {"grp": to}
            ).start()

    exchange(1, acc[...], first_picked, hand_back)
    lr[g] = ls[g]

    def own_rows(blocks):
        lines = [
            jnp.concatenate(
                [block[mg * quarter : (mg + 1) * quarter] for mg in range(4)], axis=1
            )
            for block in blocks
        ]
        return jnp.concatenate(lines, axis=0)

    here = pl.ds(pl.multiple_of(g * LANES, LANES), LANES)
    lifted = dot_nn(own_rows([af[q, :, here] for q in range(grps)]), bd[g])
    acc[...] = st[...] - relax_weight * lifted
    coarse_second(1)
    arrive("w_fin", (lr.at[pl.ds(0, grps - 1)], fin_r))
    acc[...] -= relax_weight * dot_nn(own_rows([lr[q] for q in range(grps)]), bd[g])
    pk[g] = coarse_third(1) + totals[0]
    for step in (2, 1, 3):
        remote(pk.at[g], pk.at[g], k3_s, k3_r, {"grp": grp_at(step)}).start()
    basis = jnp.concatenate([ca[g], ca[g]], axis=0)
    arrive("w_k3", (pk.at[pl.ds(0, grps - 1)], k3_r))
    tall = jnp.concatenate([pk[q].T[:quarter] for q in range(grps)], axis=0)
    corr = dot_nn(jnp.concatenate(halves(tall), axis=1), basis)
    out[...] = acc[...] - coarse_weight * corr

    others = pl.ds(0, grps - 1)
    done = [
        (tb.at[others], ag_s.at[0]),
        (af.at[others], ag_s.at[1]),
        (ca.at[others], p_s.at[0]),
        (pa.at[others], p_s.at[1]),
        (psc.at[others], p_s.at[2]),
        (ls.at[others], fin_s),
        (pk.at[others], k3_s),
    ]
    for turn in range(ITERS):
        done += [
            (sb.at[turn, others], a2a_s.at[turn]),
            (zs.at[turn, pl.ds(0, LINKS - 1)], ex_s.at[turn]),
            (rs.at[turn, pl.ds(0, LINKS - 1)], ret_s.at[turn]),
            (pz.at[turn, pl.ds(0, zs_n - 1)], k1_s.at[turn]),
            (ks.at[turn, pl.ds(0, yc_n - 1)], k2_s.at[turn]),
        ]
    with jax.named_scope("w_sends"):
        for ref, sem in done:
            whole(ref, sem).wait_send()


def solution(mesh):
    subs, grps = mesh.shape["sub"], mesh.shape["grp"]
    zs_n = 8 if subs == 128 else 2
    yc_n = subs // zs_n
    sizes = (subs, grps, zs_n, yc_n)

    def body(
        schur,
        rhs,
        start,
        project,
        coarse_basis,
        owner_of_face,
        mortar_of_face,
        mortar_order,
        subdomain_map,
        vertex_ids,
    ):
        rows, cols = schur.shape[1], schur.shape[2]
        part = cols // grps
        wide = rhs.shape[2]
        faces = owner_of_face.shape[1]
        block = LANES
        dma = pltpu.SemaphoreType.DMA
        vmem = pltpu.VMEM
        scratch = [
            vmem((grps, rows, part), BF16),
            vmem((wide, rows), F32),
            vmem((wide, rows), F32),
            vmem((grps, wide, rows), BF16),
            vmem((grps, wide, rows), BF16),
            vmem((grps,) + project.shape[1:], BF16),
            vmem((grps,) + coarse_basis.shape[1:], BF16),
            vmem((grps, rows, rows), BF16),
            vmem((4, rows, rows), BF16),
            vmem((rows, LINKS * block), BF16),
            vmem((LINKS * block, 16 * MORT_OWN), BF16),
            vmem((8, 16 * MORT_OWN), F32),
            vmem((wide, rows), F32),
            vmem((wide, rows), F32),
            vmem((ITERS, grps, wide, block), BF16),
            vmem((ITERS, grps, wide, block), BF16),
            vmem((ITERS, LINKS, wide, block), BF16),
            vmem((ITERS, LINKS, wide, block), BF16),
            vmem((ITERS, LINKS, wide, block), BF16),
            vmem((ITERS, LINKS, wide, block), BF16),
            vmem((grps, wide, block), BF16),
            vmem((grps, wide, block), BF16),
            vmem((4, 2 * NCV, rows), BF16),
            vmem((grps, 2 * NCV, rows), BF16),
            vmem((yc_n * NCV, zs_n * NCV), BF16),
            vmem((ITERS, NCV, LANES), F32),
            vmem((ITERS, zs_n, NCV, LANES), F32),
            vmem((ITERS, yc_n, NCV, LANES), F32),
            vmem((ITERS, yc_n, NCV, LANES), F32),
            vmem((grps, NCV, LANES), F32),
            vmem((faces, subs), jnp.int32),
            vmem((faces, subs), jnp.int32),
            vmem((MORT_OWN, subs), jnp.int32),
            vmem((1, subs), jnp.int32),
            vmem((NCV, subs), jnp.int32),
            dma((9 + grps,)),
            dma((2,)),
            dma((2, 2 * grps + 2)),
            dma((ITERS,)),
            dma((ITERS, PARTS)),
            dma((ITERS,)),
            dma((ITERS, PARTS)),
            dma((ITERS,)),
            dma((ITERS, PARTS)),
            dma((3,)),
            dma((3,)),
            dma((ITERS,)),
            dma((ITERS,)),
            dma((ITERS,)),
            dma((ITERS,)),
            dma(()),
            dma(()),
            dma(()),
            dma(()),
        ]
        operands = (
            schur[0],
            rhs[0].T,
            start[0].T,
            project[0],
            coarse_basis[0],
            owner_of_face[:, :, 0].T,
            mortar_of_face.T,
            mortar_order.T,
            subdomain_map.reshape(1, subs),
            vertex_ids.T,
        )
        result = pl.pallas_call(
            functools.partial(kernel, sizes),
            out_shape=jax.ShapeDtypeStruct((wide, rows), F32),
            in_specs=[pl.BlockSpec(memory_space=pltpu.HBM)] * 10,
            out_specs=pl.BlockSpec(memory_space=pltpu.VMEM),
            scratch_shapes=scratch,
            compiler_params=pltpu.CompilerParams(
                collective_id=0, has_side_effects=True, vmem_limit_bytes=44 * 1024 * 1024
            ),
        )(*(pltpu.with_memory_space_constraint(value, pltpu.HBM) for value in operands))
        return result.T[None]

    split = P("sub", "grp", None)
    return jax.shard_map(
        body,
        mesh=mesh,
        in_specs=(split, split, split, split, P("sub", None, "grp"), P(), P(), P(), P(), P()),
        out_specs=split,
        check_vma=False,
    )
```

```python
import functools

import jax
import jax.numpy as jnp
from jax import lax
from jax.experimental import pallas as pl
from jax.experimental.pallas import tpu as pltpu
from jax.sharding import PartitionSpec as P

MORT_OWN = 16
REACH = 2
LINKS = 2 * REACH + 1
HALF_LINKS = REACH + 1
CAP = 8
NCV = 8
ITERS = 2
PARTS = 2
LANES = 128
MESH = pl.DeviceIdType.MESH
HIGHEST = lax.Precision.HIGHEST
F32 = jnp.float32
BF16 = jnp.bfloat16

relax_weight = 0.5
coarse_weight = 0.5


def iota(shape, dim):
    return lax.broadcasted_iota(jnp.int32, shape, dim)


def dot_nn(a, b):
    return lax.dot_general(a, b, (((1,), (0,)), ((), ())), preferred_element_type=F32)


def dot_nt(a, b):
    return lax.dot_general(a, b, (((1,), (1,)), ((), ())), preferred_element_type=F32)


def halves(x):
    high = x.astype(BF16)
    return high, (x - high.astype(F32)).astype(BF16)


def kernel(
    sizes,
    schur,
    rhs,
    start,
    project,
    coarse,
    owner_t,
    mortar_t,
    order_t,
    holder,
    vertex_t,
    out,
    s4,
    st,
    rh,
    tb,
    af,
    pa,
    ca,
    bd,
    sp,
    wm,
    vm,
    fac,
    acc,
    prod,
    sb,
    ar,
    zs,
    orr,
    rs,
    rr,
    ls,
    lr,
    qm,
    qs,
    qr,
    gm,
    av,
    psc,
    dm,
    ps,
    pz,
    ks,
    kr,
    pk,
    own_tab,
    mor_tab,
    ord_tab,
    hol_tab,
    ver_tab,
    lsem,
    ag_s,
    ag_r,
    a2a_s,
    a2a_r,
    ex_s,
    ex_r,
    ret_s,
    ret_r,
    p_s,
    p_r,
    k1_s,
    k1_r,
    k2_s,
    k2_r,
    k3_s,
    k3_r,
    fin_s,
    fin_r,
):
    subs, grps, zs_n, yc_n = sizes
    s = lax.axis_index("sub")
    g = lax.axis_index("grp")
    z = s // yc_n
    yc = lax.rem(s, yc_n)
    cols = s4.shape[2]
    quarter = tb.shape[1] // grps
    half = tb.shape[1] // 2

    def sub_at(step):
        return lax.rem(s + step + subs, subs)

    def grp_at(step):
        return lax.rem(g + step, grps)

    def remote(src, dst, send, recv, where):
        return pltpu.make_async_remote_copy(
            src_ref=src,
            dst_ref=dst,
            send_sem=send,
            recv_sem=recv,
            device_id=where,
            device_id_type=MESH,
        )

    def whole(ref, sem):
        return remote(ref, ref, sem, sem, {"grp": grp_at(1)})

    def arrive(name, *parts):
        with jax.named_scope(name):
            for ref, sem in parts:
                whole(ref, sem).wait_recv()

    loads = [
        pltpu.make_async_copy(start, st, lsem.at[0]),
        pltpu.make_async_copy(owner_t, own_tab, lsem.at[1]),
        pltpu.make_async_copy(mortar_t, mor_tab, lsem.at[2]),
        pltpu.make_async_copy(order_t, ord_tab, lsem.at[3]),
        pltpu.make_async_copy(holder, hol_tab, lsem.at[4]),
        pltpu.make_async_copy(vertex_t, ver_tab, lsem.at[5]),
        pltpu.make_async_copy(project, pa.at[g], lsem.at[6]),
        pltpu.make_async_copy(coarse, ca.at[g], lsem.at[7]),
        pltpu.make_async_copy(rhs, rh, lsem.at[8]),
    ]
    for q in range(grps):
        loads.append(
            pltpu.make_async_copy(
                schur.at[:, pl.ds(q * cols, cols)], s4.at[q], lsem.at[9 + q]
            )
        )
    loads[0].start()

    barrier = pltpu.get_barrier_semaphore()
    partners = [{"sub": lax.rem(z + step, zs_n) * yc_n + yc} for step in range(1, zs_n)]
    partners += [{"sub": z * yc_n + lax.rem(yc + step, yc_n)} for step in range(1, yc_n)]
    partners += [{"sub": sub_at(step)} for step in (-2, -1, 1, 2)]
    partners += [{"grp": grp_at(step)} for step in range(1, grps)]
    for where in partners:
        pl.semaphore_signal(barrier, inc=1, device_id=where, device_id_type=MESH)

    for load in loads[1:]:
        load.start()

    with jax.named_scope("w_start"):
        loads[0].wait()
    tb[g] = st[...].astype(BF16)
    with jax.named_scope("w_barrier"):
        pl.semaphore_wait(barrier, len(partners))

    left, right = grp_at(grps - 1), grp_at(1)
    across = grp_at(2)
    to_right, to_left = {"grp": right}, {"grp": left}

    def gather_plan(buf, turn):
        def piece(q, i):
            return buf.at[q, pl.ds(i * quarter, quarter)]

        def send(q, i, place, where):
            ref = piece(q, i)
            remote(ref, ref, ag_s.at[turn], ag_r.at[turn, place], where).start()

        far = [2 * grps + turn * (i // 2) for i in range(grps)]
        return piece, send, far

    def gather_send(plan, i):
        _, send, _ = plan
        send(g, i, i, to_right)
        send(g, i + 1, grps + i + 1, to_left)
        send(g, i + 1, i + 1, to_right)
        send(g, i, grps + i, to_left)

    def from_left(plan, turn, i):
        return plan[0](left, i), ag_r.at[turn, i]

    def from_right(plan, turn, i):
        return plan[0](right, i), ag_r.at[turn, grps + i]

    def gather_forward(plan, turn, i):
        _, send, far = plan
        if i % 2:
            arrive("w_near", from_right(plan, turn, i))
            send(right, i, far[i], to_left)
        else:
            arrive("w_near", from_left(plan, turn, i))
            send(left, i, far[i], to_right)

    gathered = gather_plan(tb, 0)
    for i in range(0, grps, 2):
        gather_send(gathered, i)

    for load in loads[1:6]:
        load.wait()
    stacked = jnp.concatenate(
        [own_tab[...].astype(F32), mor_tab[...].astype(F32), ver_tab[...].astype(F32)], axis=0
    ).astype(BF16)
    placed = jnp.where(
        iota((subs, subs), 0) == jnp.broadcast_to(hol_tab[...], (subs, subs)), 1.0, 0.0
    ).astype(BF16)
    moved = dot_nn(stacked, placed)
    faces = own_tab.shape[0]
    held_all, mortar_all = moved[:faces], moved[faces : 2 * faces]
    vertex_all = moved[2 * faces :]

    def column(table, index):
        mask = iota(table.shape, 1) == index
        return jnp.sum(jnp.where(mask, table, 0.0), axis=1, keepdims=True)

    square_i, square_j = iota((faces, faces), 0), iota((faces, faces), 1)

    def as_row(col):
        return jnp.sum(jnp.where(square_i == square_j, col, 0.0), axis=0, keepdims=True)

    held_c = column(held_all, s)
    held_r = as_row(held_c)
    rank_r = jnp.sum(
        jnp.where((held_c == held_r) & (square_i < square_j), 1.0, 0.0), axis=0, keepdims=True
    )
    slot_r = held_r * CAP + rank_r
    rows = iota((wm.shape[0], faces), 0)
    face_of = jnp.left_shift(jnp.right_shift(rows, 7), 3) | (rows & 7)
    slot_c = jnp.sum(
        jnp.where(iota(rows.shape, 1) == face_of, slot_r, 0.0), axis=1, keepdims=True
    )
    r_i, c_i = iota(wm.shape, 0), iota(wm.shape, 1)
    same = (jnp.right_shift(r_i, 3) & 15) == (jnp.right_shift(c_i, 3) & 15)
    slot_of = (jnp.left_shift(jnp.right_shift(c_i, 7), 3) | (c_i & 7)).astype(F32)
    wm[...] = jnp.where(same & (slot_c == slot_of), 1.0, 0.0).astype(BF16)

    width = vm.shape[1]
    lane8 = iota((faces, CAP), 1).astype(F32)
    pick8 = iota((LANES, CAP), 1) == (iota((LANES, CAP), 0) & 7)
    v_r, v_c = iota((LANES, width), 0), iota((LANES, width), 1)
    v_same = jnp.right_shift(v_r, 3) == jnp.right_shift(v_c, 4)
    v_key = (v_c & 15).astype(F32)
    counts = jnp.zeros((1, width), F32)
    for link in range(LINKS):
        sender = sub_at(REACH - link)
        hc, mc = column(held_all, sender), column(mortar_all, sender)
        hr = as_row(hc)
        rank_c = jnp.sum(
            jnp.where((hr == hc) & (square_j < square_i), 1.0, 0.0), axis=1, keepdims=True
        )
        key8 = (
            jnp.sum(
                jnp.where((hc == float(link)) & (rank_c == lane8), mc + 1.0, 0.0),
                axis=0,
                keepdims=True,
            )
            - 1.0
        )
        key_c = jnp.sum(jnp.where(pick8, key8, 0.0), axis=1, keepdims=True)
        block = jnp.where(v_same & (key_c == v_key), 1.0, 0.0)
        counts = counts + jnp.sum(block, axis=0, keepdims=True)
        vm[pl.ds(link * LANES, LANES), :] = block.astype(BF16)
    order_c = column(ord_tab[...].astype(F32), s)
    order_r = jnp.sum(
        jnp.where(iota((MORT_OWN, width), 0) == (iota((MORT_OWN, width), 1) & 15), order_c, 0.0),
        axis=0,
        keepdims=True,
    )
    inverse = 1.0 / jnp.maximum(counts, 1.0)
    row_c = iota((1, width), 1)
    for mg in range(4):
        first = (2 * mg + jnp.right_shift(row_c, 7)).astype(F32)
        second = (jnp.right_shift(row_c, 4) & 7).astype(F32)
        keep = (first <= order_r) & (second <= order_r)
        fac[pl.ds(mg, 1), :] = jnp.where(keep, inverse, 0.0)

    vertex_b = vertex_all.astype(BF16)
    d_rows, d_cols = dm.shape[0] // 2, dm.shape[1]
    here = jnp.where(
        iota((d_rows, subs), 1) == z * yc_n + jnp.right_shift(iota((d_rows, subs), 0), 3), 1.0, 0.0
    ).astype(BF16)
    wanted = dot_nt(here, vertex_b)
    wanted = jnp.sum(
        jnp.where(iota((d_rows, NCV), 1) == (iota((d_rows, NCV), 0) & 7), wanted, 0.0),
        axis=1,
        keepdims=True,
    )
    block = zs_n * NCV
    places = iota((subs, block), 0)
    corner = iota((subs, block), 1)
    met = []
    for link in range(LINKS):
        sender = jnp.right_shift(corner, 3) * yc_n + yc + (subs + REACH - link)
        there = jnp.where(places == (sender & (subs - 1)), 1.0, 0.0).astype(BF16)
        given = dot_nn(vertex_b, there)
        given = jnp.sum(
            jnp.where(iota((NCV, block), 0) == (iota((NCV, block), 1) & 7), given, 0.0),
            axis=0,
            keepdims=True,
        )
        met.append(jnp.where(wanted == given, 1.0, 0.0))
    met.append(jnp.zeros_like(met[0]))
    for i in range(HALF_LINKS):
        for side in range(2):
            dm[pl.ds(side * d_rows, d_rows), pl.ds(i * block, block)] = met[
                side * HALF_LINKS + i
            ].astype(BF16)

    lane = iota((CAP, LANES), 1)
    row8 = iota((CAP, 4 * LANES), 0)
    own_face = row8 == jnp.right_shift(iota((CAP, 4 * LANES), 1), 6)

    def build_block(q):
        def step(i, carry):
            pair = pa[q, :, pl.ds(pl.multiple_of(i * LANES, LANES), LANES)].astype(F32)
            turned = pltpu.roll(pair, LANES // 2, 1)
            even = jnp.where(lane < LANES // 2, pair, turned)
            odd = jnp.where(lane < LANES // 2, turned, pair)
            even = jnp.where(own_face, jnp.concatenate([even] * 4, axis=1), 0.0)
            odd = jnp.where(own_face, jnp.concatenate([odd] * 4, axis=1), 0.0)
            both = jnp.concatenate([even, odd], axis=0).astype(BF16)
            bd[q, pl.ds(pl.multiple_of(i * 16, 16), 16), :] = both
            return carry

        lax.fori_loop(0, pa.shape[2] // LANES, step, 0, unroll=8)

    def fold_block(q, s_block):
        wide = dot_nt(s_block, bd[q]).astype(BF16)
        for mg in range(4):
            sp[mg, :, pl.ds(pl.multiple_of(q * LANES, LANES), LANES)] = wide[
                :, mg * LANES : (mg + 1) * LANES
            ]

    def fold_coarse():
        both = jnp.concatenate(halves(dot_nt(ca[g], bd[g])), axis=0)
        for mg in range(4):
            qm[g, pl.ds(mg * 2 * NCV, 2 * NCV), :] = both[:, mg * LANES : (mg + 1) * LANES]

    loads[6].wait()
    loads[7].wait()
    with jax.named_scope("c_block"):
        build_block(g)
    with jax.named_scope("w_loads"):
        for load in loads[8:]:
            load.wait()
    for i in range(grps):
        gather_forward(gathered, 0, i)
    fold_coarse()
    for i, ref in enumerate((ca, qm)):
        for step in (2, 1, 3):
            where = {"grp": grp_at(step)}
            remote(ref.at[g], ref.at[g], p_s.at[i], p_r.at[i], where).start()

    def add_block(q):
        acc[...] += dot_nt(tb[q], s4[q])

    acc[...] = dot_nt(tb[g], s4[g])
    arrive("w_left", from_left(gathered, 0, 1), from_left(gathered, 0, 3))
    add_block(left)
    arrive("w_right", from_right(gathered, 0, 0), from_right(gathered, 0, 2))
    add_block(right)
    arrive("w_across", (tb.at[across], ag_r.at[0, 2 * grps]))
    add_block(across)
    prod[...] = acc[...] - rh[...]

    groups = 4 // PARTS
    span = groups * quarter

    def rows_of(part):
        return pl.ds(part * span, span)

    def swap_out(turn, part, q):
        remote(
            sb.at[turn, q, rows_of(part)],
            ar.at[turn, g, rows_of(part)],
            a2a_s.at[turn],
            a2a_r.at[turn, part],
            {"grp": q},
        ).start()

    def swap_all(residual):
        residual = residual.astype(BF16)
        for part in range(PARTS):
            first = part * groups
            modes = bd[g, pl.ds(first * LANES, groups * LANES), :]
            coeffs = dot_nt(residual, modes).astype(BF16)
            for q in range(grps):
                for mg in range(groups):
                    sb[0, q, pl.ds((first + mg) * quarter, quarter), :] = coeffs[
                        q * quarter : (q + 1) * quarter, mg * LANES : (mg + 1) * LANES
                    ]
            for step in (2, 1, 3):
                swap_out(0, part, grp_at(step))
        ar[0, g] = sb[0, g]

    def swap_quarter(q, own):
        at = pl.ds(pl.multiple_of(q * quarter, quarter), quarter)
        coeffs = dot_nt(acc[at, :].astype(BF16), bd[g]).astype(BF16)
        tall = jnp.concatenate(
            [coeffs[:, mg * LANES : (mg + 1) * LANES] for mg in range(4)], axis=0
        )
        if own:
            ar[1, g] = tall
            return
        sb[1, q] = tall
        for part in range(PARTS):
            swap_out(1, part, q)

    def exchange(turn, picked, deliver):
        partials = []
        if turn == 0:
            for step in (2, 1, 3):
                where = {"grp": grp_at(step)}
                remote(pa.at[g], pa.at[g], p_s.at[4], p_r.at[4], where).start()
            others = pl.ds(0, grps - 1)
            fold_block(g, s4[g])
            arrive("w_extra", (ca.at[others], p_r.at[0]), (qm.at[others], p_r.at[1]))
            slots = dot_nn(
                jnp.concatenate([qm[q] for q in range(grps)], axis=1), wm[...]
            ).astype(BF16)
            for link in (0, 4, 1, 3, 2):
                piece = slots[:, link * LANES : (link + 1) * LANES]
                if link == REACH:
                    qr[link] = piece
                    continue
                qs[link] = piece
        terms = None if picked is None else picked()
        for part in range(PARTS):
            arrive("w_a2a", (ar.at[turn, pl.ds(0, grps - 1), rows_of(part)], a2a_r.at[turn, part]))
            lines = [ar[turn, q, rows_of(part), :] for q in range(grps)]
            if terms is not None:
                for q in range(grps):
                    tall = jnp.concatenate(
                        [
                            terms[q][:, mg * LANES : (mg + 1) * LANES]
                            for mg in range(part * groups, (part + 1) * groups)
                        ],
                        axis=0,
                    )
                    lines[q] = (lines[q].astype(F32) - coarse_weight * tall).astype(BF16)
            grouped = dot_nn(jnp.concatenate(lines, axis=1), wm[...]).astype(BF16)
            for link in (0, 4, 1, 3, 2):
                piece = grouped[:, link * LANES : (link + 1) * LANES]
                if link == REACH:
                    orr[turn, link, rows_of(part), :] = piece
                    continue
                zs[turn, link, rows_of(part), :] = piece
                remote(
                    zs.at[turn, link, rows_of(part)],
                    orr.at[turn, link, rows_of(part)],
                    ex_s.at[turn],
                    ex_r.at[turn, part],
                    {"sub": sub_at(link - REACH)},
                ).start()
        if turn == 0:
            for link in (0, 4, 1, 3):
                where = {"sub": sub_at(link - REACH)}
                remote(qs.at[link], qr.at[link], p_s.at[3], p_r.at[3], where).start()
            arrive("w_p", (pa.at[others], p_r.at[4]))
            for i in range(grps - 1):
                build_block(grp_at(i + 1))
        for part in range(PARTS):
            arrive("w_ex", (orr.at[turn, pl.ds(0, LINKS - 1), rows_of(part)], ex_r.at[turn, part]))
            joined = jnp.concatenate(
                [orr[turn, link, rows_of(part), :] for link in range(LINKS)], axis=1
            )
            sums = dot_nn(joined, vm[...])
            averages = jnp.concatenate(
                [
                    sums[mg * quarter : (mg + 1) * quarter]
                    * fac[pl.ds(part * groups + mg, 1), :]
                    for mg in range(groups)
                ],
                axis=0,
            ).astype(BF16)
            replies = dot_nt(averages, vm[...]).astype(BF16)
            for link in (0, 4, 1, 3, 2):
                piece = replies[:, link * LANES : (link + 1) * LANES]
                if link == REACH:
                    rr[turn, link, rows_of(part), :] = piece
                    continue
                rs[turn, link, rows_of(part), :] = piece
                remote(
                    rs.at[turn, link, rows_of(part)],
                    rr.at[turn, link, rows_of(part)],
                    ret_s.at[turn],
                    ret_r.at[turn, part],
                    {"sub": sub_at(REACH - link)},
                ).start()
            if turn == 0:
                av[rows_of(part), :] = averages
            else:
                partials.append(coarse_part(part, averages))
        if turn == 1:
            coarse_first(1, sum(partials[1:], partials[0]))
            lift_first()
            coarse_second(1)
        if turn == 0:
            for i in range(grps - 1):
                q = grp_at(i + 1)
                fold_block(q, s4[q])
            spread = dot_nt(ca[0], s4[0])
            for q in range(1, grps):
                spread = spread + dot_nt(ca[q], s4[q])
            high, rest = halves(spread)
            psc[g] = jnp.concatenate(
                halves(dot_nt(high, bd[g]) + dot_nt(rest, bd[g])), axis=0
            )
            for step in (2, 1, 3):
                where = {"grp": grp_at(step)}
                remote(psc.at[g], psc.at[g], p_s.at[2], p_r.at[2], where).start()
            arrive("w_q", (qr.at[pl.ds(0, LINKS - 1)], p_r.at[3]))
            build_owner()
            partials = [coarse_part(part, av[rows_of(part), :]) for part in range(PARTS)]
            coarse_first(0, sum(partials[1:], partials[0]))
        for part in range(PARTS):
            arrive("w_ret", (rr.at[turn, pl.ds(0, LINKS - 1), rows_of(part)], ret_r.at[turn, part]))
            answered = jnp.concatenate(
                [rr[turn, link, rows_of(part), :] for link in range(LINKS)], axis=1
            )
            deliver(part, dot_nt(answered, wm[...]).astype(BF16))

    def build_owner():
        lines = []
        for link in range(LINKS):
            both = dot_nn(qr[link], vm[pl.ds(link * LANES, LANES), :])
            lines.append(
                [
                    both[mg * 2 * NCV : mg * 2 * NCV + NCV]
                    + both[mg * 2 * NCV + NCV : (mg + 1) * 2 * NCV]
                    for mg in range(4)
                ]
            )
        for mg in range(4):
            full = jnp.concatenate([line[mg] for line in lines], axis=0)
            gm[mg] = jnp.concatenate(halves(full), axis=0)

    def coarse_part(part, averages):
        gap = jnp.zeros((LANES // 2 - quarter, averages.shape[1]), BF16)
        total = None
        for mg in range(groups):
            line = averages[mg * quarter : (mg + 1) * quarter]
            twice = jnp.concatenate([line, gap, line, gap], axis=0)
            value = dot_nt(gm[part * groups + mg], twice)
            total = value if total is None else total + value
        return total[: LINKS * NCV] + total[LINKS * NCV :]

    side = iota((HALF_LINKS * NCV, LANES), 1) < LANES // 2

    def coarse_first(turn, value):
        first = value[: HALF_LINKS * NCV]
        second = jnp.concatenate(
            [value[HALF_LINKS * NCV :], jnp.zeros((NCV, LANES), F32)], axis=0
        )
        ps[turn] = jnp.where(side, first, second).astype(BF16)
        for step in range(zs_n - 1):
            to = lax.rem(z + step + 1, zs_n) * yc_n + yc
            remote(
                ps.at[turn], pz.at[turn, z], k1_s.at[turn], k1_r.at[turn], {"sub": to}
            ).start()
        pz[turn, z] = ps[turn]

    def coarse_second(turn):
        arrive("w_k1", (pz.at[turn, pl.ds(0, zs_n - 1)], k1_r.at[turn]))
        near = pz[turn].astype(F32)
        lines = jnp.concatenate(
            [
                near[:, i * NCV : (i + 1) * NCV, :].reshape(zs_n * NCV, LANES)
                for i in range(HALF_LINKS)
            ],
            axis=0,
        ).astype(BF16)
        value = dot_nn(dm[...], lines)
        half_rows = value.shape[0] // 2
        lane_of = iota((half_rows, LANES), 1)
        value = jnp.where(lane_of < LANES // 2, value[:half_rows], value[half_rows:])
        ks[turn] = value.reshape(yc_n, NCV, LANES)
        for step in range(yc_n - 1):
            to = lax.rem(yc + step + 1, yc_n)
            remote(
                ks.at[turn, to],
                kr.at[turn, yc],
                k2_s.at[turn],
                k2_r.at[turn],
                {"sub": z * yc_n + to},
            ).start()
        kr[turn, yc] = ks[turn, yc]

    def coarse_third(turn):
        arrive("w_k2", (kr.at[turn, pl.ds(0, yc_n - 1)], k2_r.at[turn]))
        total = jnp.sum(kr[turn], axis=0)
        return total + pltpu.roll(total, LANES // 2, 1)

    gathered = gather_plan(af, 1)
    def spread_out(part, mine):
        af[g, rows_of(part), :] = mine
        for i in range(part * groups, (part + 1) * groups, 2):
            gather_send(gathered, i)

    swap_all(prod[...])
    exchange(0, None, spread_out)

    def add_modes(q, groups_of, fresh):
        at = pl.ds(pl.multiple_of(q * quarter, quarter), quarter)
        value = dot_nt(af[q, pl.ds(groups_of[0] * quarter, quarter), :], sp[groups_of[0]])
        for mg in groups_of[1:]:
            value = value + dot_nt(af[q, pl.ds(mg * quarter, quarter), :], sp[mg])
        base = prod if fresh else acc
        acc[at, :] = base[at, :] - relax_weight * value

    add_modes(g, (0, 1, 2, 3), True)
    swap_quarter(g, True)
    gather_forward(gathered, 1, 0)
    gather_forward(gathered, 1, 1)
    arrive("w_left", from_left(gathered, 1, 1))
    add_modes(left, (0, 1), True)
    arrive("w_right", from_right(gathered, 1, 0))
    add_modes(right, (0, 1), True)
    coarse_second(0)
    gather_forward(gathered, 1, 2)
    gather_forward(gathered, 1, 3)
    arrive("w_left", from_left(gathered, 1, 3))
    add_modes(left, (2, 3), False)
    swap_quarter(left, False)
    arrive("w_right", from_right(gathered, 1, 2))
    add_modes(right, (2, 3), False)
    swap_quarter(right, False)
    for part in range(2):
        far = af.at[across, pl.ds(2 * part * quarter, 2 * quarter)]
        arrive("w_across", (far, ag_r.at[1, 2 * grps + part]))
        add_modes(across, (2 * part, 2 * part + 1), part == 0)
    swap_quarter(across, False)
    totals = []

    def first_picked():
        arrive("w_psc", (psc.at[pl.ds(0, grps - 1)], p_r.at[2]))
        picked = coarse_third(0)
        totals.append(picked)
        high, rest = halves(picked.T[:quarter])
        both = jnp.concatenate(
            [jnp.concatenate([high, high], axis=1), jnp.concatenate([rest, rest], axis=1)],
            axis=0,
        )
        terms = []
        for q in range(grps):
            term = dot_nn(both, psc[q])
            terms.append(term[:quarter] + term[quarter:])
        return terms

    def hand_back(part, mine):
        for q in range(grps):
            ls[q, rows_of(part), :] = mine[:, q * LANES : (q + 1) * LANES]
        for step in (2, 1, 3):
            to = grp_at(step)
            remote(
                ls.at[to, rows_of(part)], lr.at[g, rows_of(part)], fin_s, fin_r, {"grp": to}
            ).start()

    def own_rows(blocks):
        lines = [
            jnp.concatenate(
                [block[mg * quarter : (mg + 1) * quarter] for mg in range(4)], axis=1
            )
            for block in blocks
        ]
        return jnp.concatenate(lines, axis=0)

    def lift_first():
        here = pl.ds(pl.multiple_of(g * LANES, LANES), LANES)
        lifted = dot_nn(own_rows([af[q, :, here] for q in range(grps)]), bd[g])
        acc[...] = st[...] - relax_weight * lifted

    exchange(1, first_picked, hand_back)
    lr[g] = ls[g]
    pk[g] = coarse_third(1) + totals[0]
    for step in (2, 1, 3):
        remote(pk.at[g], pk.at[g], k3_s, k3_r, {"grp": grp_at(step)}).start()
    arrive("w_fin", (lr.at[pl.ds(0, grps - 1)], fin_r))
    acc[...] -= relax_weight * dot_nn(own_rows([lr[q] for q in range(grps)]), bd[g])
    basis = jnp.concatenate([ca[g], ca[g]], axis=0)
    arrive("w_k3", (pk.at[pl.ds(0, grps - 1)], k3_r))
    tall = jnp.concatenate([pk[q].T[:quarter] for q in range(grps)], axis=0)
    corr = dot_nn(jnp.concatenate(halves(tall), axis=1), basis)
    out[...] = acc[...] - coarse_weight * corr

    others = pl.ds(0, grps - 1)
    done = [
        (tb.at[others], ag_s.at[0]),
        (af.at[others], ag_s.at[1]),
        (ca.at[others], p_s.at[0]),
        (qm.at[others], p_s.at[1]),
        (pa.at[others], p_s.at[4]),
        (psc.at[others], p_s.at[2]),
        (qs.at[pl.ds(0, LINKS - 1)], p_s.at[3]),
        (ls.at[others], fin_s),
        (pk.at[others], k3_s),
    ]
    for turn in range(ITERS):
        done += [
            (sb.at[turn, others], a2a_s.at[turn]),
            (zs.at[turn, pl.ds(0, LINKS - 1)], ex_s.at[turn]),
            (rs.at[turn, pl.ds(0, LINKS - 1)], ret_s.at[turn]),
            (pz.at[turn, pl.ds(0, zs_n - 1)], k1_s.at[turn]),
            (ks.at[turn, pl.ds(0, yc_n - 1)], k2_s.at[turn]),
        ]
    with jax.named_scope("w_sends"):
        for ref, sem in done:
            whole(ref, sem).wait_send()


def solution(mesh):
    subs, grps = mesh.shape["sub"], mesh.shape["grp"]
    zs_n = 8 if subs == 128 else 2
    yc_n = subs // zs_n
    sizes = (subs, grps, zs_n, yc_n)

    def body(
        schur,
        rhs,
        start,
        project,
        coarse_basis,
        owner_of_face,
        mortar_of_face,
        mortar_order,
        subdomain_map,
        vertex_ids,
    ):
        rows, cols = schur.shape[1], schur.shape[2]
        part = cols // grps
        wide = rhs.shape[2]
        faces = owner_of_face.shape[1]
        block = LANES
        dma = pltpu.SemaphoreType.DMA
        vmem = pltpu.VMEM
        scratch = [
            vmem((grps, rows, part), BF16),
            vmem((wide, rows), F32),
            vmem((wide, rows), F32),
            vmem((grps, wide, rows), BF16),
            vmem((grps, wide, rows), BF16),
            vmem((grps,) + project.shape[1:], BF16),
            vmem((grps,) + coarse_basis.shape[1:], BF16),
            vmem((grps, rows, rows), BF16),
            vmem((4, rows, rows), BF16),
            vmem((rows, LINKS * block), BF16),
            vmem((LINKS * block, 16 * MORT_OWN), BF16),
            vmem((8, 16 * MORT_OWN), F32),
            vmem((wide, rows), F32),
            vmem((wide, rows), F32),
            vmem((ITERS, grps, wide, block), BF16),
            vmem((ITERS, grps, wide, block), BF16),
            vmem((ITERS, LINKS, wide, block), BF16),
            vmem((ITERS, LINKS, wide, block), BF16),
            vmem((ITERS, LINKS, wide, block), BF16),
            vmem((ITERS, LINKS, wide, block), BF16),
            vmem((grps, wide, block), BF16),
            vmem((grps, wide, block), BF16),
            vmem((grps, 8 * NCV, block), BF16),
            vmem((LINKS, 8 * NCV, block), BF16),
            vmem((LINKS, 8 * NCV, block), BF16),
            vmem((4, 2 * LINKS * NCV, 16 * MORT_OWN), BF16),
            vmem((wide, 16 * MORT_OWN), BF16),
            vmem((grps, 2 * NCV, rows), BF16),
            vmem((2 * yc_n * NCV, HALF_LINKS * zs_n * NCV), BF16),
            vmem((ITERS, HALF_LINKS * NCV, LANES), BF16),
            vmem((ITERS, zs_n, HALF_LINKS * NCV, LANES), BF16),
            vmem((ITERS, yc_n, NCV, LANES), F32),
            vmem((ITERS, yc_n, NCV, LANES), F32),
            vmem((grps, NCV, LANES), F32),
            vmem((faces, subs), jnp.int32),
            vmem((faces, subs), jnp.int32),
            vmem((MORT_OWN, subs), jnp.int32),
            vmem((1, subs), jnp.int32),
            vmem((NCV, subs), jnp.int32),
            dma((9 + grps,)),
            dma((2,)),
            dma((2, 2 * grps + 2)),
            dma((ITERS,)),
            dma((ITERS, PARTS)),
            dma((ITERS,)),
            dma((ITERS, PARTS)),
            dma((ITERS,)),
            dma((ITERS, PARTS)),
            dma((5,)),
            dma((5,)),
            dma((ITERS,)),
            dma((ITERS,)),
            dma((ITERS,)),
            dma((ITERS,)),
            dma(()),
            dma(()),
            dma(()),
            dma(()),
        ]
        operands = (
            schur[0],
            rhs[0].T,
            start[0].T,
            project[0],
            coarse_basis[0],
            owner_of_face[:, :, 0].T,
            mortar_of_face.T,
            mortar_order.T,
            subdomain_map.reshape(1, subs),
            vertex_ids.T,
        )
        result = pl.pallas_call(
            functools.partial(kernel, sizes),
            out_shape=jax.ShapeDtypeStruct((wide, rows), F32),
            in_specs=[pl.BlockSpec(memory_space=pltpu.HBM)] * 10,
            out_specs=pl.BlockSpec(memory_space=pltpu.VMEM),
            scratch_shapes=scratch,
            compiler_params=pltpu.CompilerParams(
                collective_id=0, has_side_effects=True, vmem_limit_bytes=44 * 1024 * 1024
            ),
        )(*(pltpu.with_memory_space_constraint(value, pltpu.HBM) for value in operands))
        return result.T[None]

    split = P("sub", "grp", None)
    return jax.shard_map(
        body,
        mesh=mesh,
        in_specs=(split, split, split, split, P("sub", None, "grp"), P(), P(), P(), P(), P()),
        out_specs=split,
        check_vma=False,
    )
```

```python
import functools

import jax
import jax.numpy as jnp
from jax import lax
from jax.experimental import pallas as pl
from jax.experimental.pallas import tpu as pltpu
from jax.sharding import PartitionSpec as P

MORT_OWN = 16
REACH = 2
LINKS = 2 * REACH + 1
HALF_LINKS = REACH + 1
CAP = 8
NCV = 8
ITERS = 2
PARTS = 2
LANES = 128
MESH = pl.DeviceIdType.MESH
HIGHEST = lax.Precision.HIGHEST
F32 = jnp.float32
BF16 = jnp.bfloat16

relax_weight = 0.5
coarse_weight = 0.5


def iota(shape, dim):
    return lax.broadcasted_iota(jnp.int32, shape, dim)


def dot_nn(a, b):
    return lax.dot_general(a, b, (((1,), (0,)), ((), ())), preferred_element_type=F32)


def dot_nt(a, b):
    return lax.dot_general(a, b, (((1,), (1,)), ((), ())), preferred_element_type=F32)


def halves(x):
    high = x.astype(BF16)
    return high, (x - high.astype(F32)).astype(BF16)


def kernel(
    sizes,
    schur,
    rhs,
    start,
    project,
    coarse,
    owner_t,
    mortar_t,
    order_t,
    holder,
    vertex_t,
    out,
    s4,
    st,
    rh,
    tb,
    af,
    pa,
    ca,
    bd,
    sp,
    wm,
    vm,
    fac,
    acc,
    prod,
    sb,
    ar,
    zs,
    orr,
    rs,
    rr,
    ls,
    lr,
    qm,
    qs,
    qr,
    gm,
    av,
    psc,
    dm,
    ps,
    pz,
    ks,
    kr,
    pk,
    own_tab,
    mor_tab,
    ord_tab,
    hol_tab,
    ver_tab,
    lsem,
    ag_s,
    ag_r,
    a2a_s,
    a2a_r,
    ex_s,
    ex_r,
    ret_s,
    ret_r,
    p_s,
    p_r,
    k1_s,
    k1_r,
    k2_s,
    k2_r,
    k3_s,
    k3_r,
    fin_s,
    fin_r,
    news,
):
    subs, grps, zs_n, yc_n = sizes
    s = lax.axis_index("sub")
    g = lax.axis_index("grp")
    z = s // yc_n
    yc = lax.rem(s, yc_n)
    cols = s4.shape[2]
    quarter = tb.shape[1] // grps
    half = tb.shape[1] // 2

    def sub_at(step):
        return lax.rem(s + step + subs, subs)

    def grp_at(step):
        return lax.rem(g + step, grps)

    def remote(src, dst, send, recv, where):
        return pltpu.make_async_remote_copy(
            src_ref=src,
            dst_ref=dst,
            send_sem=send,
            recv_sem=recv,
            device_id=where,
            device_id_type=MESH,
        )

    def whole(ref, sem):
        return remote(ref, ref, sem, sem, {"grp": grp_at(1)})

    def arrive(name, *parts):
        with jax.named_scope(name):
            for ref, sem in parts:
                whole(ref, sem).wait_recv()

    loads = [
        pltpu.make_async_copy(start, st, lsem.at[0]),
        pltpu.make_async_copy(owner_t, own_tab, lsem.at[1]),
        pltpu.make_async_copy(mortar_t, mor_tab, lsem.at[2]),
        pltpu.make_async_copy(order_t, ord_tab, lsem.at[3]),
        pltpu.make_async_copy(holder, hol_tab, lsem.at[4]),
        pltpu.make_async_copy(vertex_t, ver_tab, lsem.at[5]),
        pltpu.make_async_copy(project, pa.at[g], lsem.at[6]),
        pltpu.make_async_copy(coarse, ca.at[g], lsem.at[7]),
        pltpu.make_async_copy(rhs, rh, lsem.at[8]),
    ]
    for q in range(grps):
        loads.append(
            pltpu.make_async_copy(
                schur.at[:, pl.ds(q * cols, cols)], s4.at[q], lsem.at[9 + q]
            )
        )
    loads[0].start()

    barrier = pltpu.get_barrier_semaphore()
    line = [{"sub": lax.rem(z + step, zs_n) * yc_n + yc} for step in (1, zs_n - 1)]
    plane = [
        {"sub": z * yc_n + lax.rem(yc + step, yc_n)} for step in (2, yc_n - 2)
    ]
    cross = yc - lax.rem(yc, 2) + 1 - lax.rem(yc, 2)
    mates = [{"sub": z * yc_n + lax.rem(cross + step, yc_n)} for step in (0, 2, yc_n - 2)]
    partners = line + plane + mates
    partners += [{"sub": sub_at(step)} for step in (-2, -1, 1, 2)]
    partners += [{"grp": grp_at(step)} for step in range(1, grps)]
    for where in partners:
        pl.semaphore_signal(barrier, inc=1, device_id=where, device_id_type=MESH)

    for load in loads[1:]:
        load.start()

    with jax.named_scope("w_start"):
        loads[0].wait()
    tb[g] = st[...].astype(BF16)
    with jax.named_scope("w_barrier"):
        pl.semaphore_wait(barrier, len(partners))

    left, right = grp_at(grps - 1), grp_at(1)
    across = grp_at(2)
    to_right, to_left = {"grp": right}, {"grp": left}

    def gather_plan(buf, turn):
        def piece(q, i):
            return buf.at[q, pl.ds(i * quarter, quarter)]

        def send(q, i, place, where):
            ref = piece(q, i)
            remote(ref, ref, ag_s.at[turn], ag_r.at[turn, place], where).start()

        far = [2 * grps + turn * (i // 2) for i in range(grps)]
        return piece, send, far

    def gather_send(plan, i):
        _, send, _ = plan
        send(g, i, i, to_right)
        send(g, i + 1, grps + i + 1, to_left)

    def gather_rest(plan):
        _, send, _ = plan
        for i in range(0, grps, 2):
            send(g, i + 1, i + 1, to_right)
            send(g, i, grps + i, to_left)

    def from_left(plan, turn, i):
        return plan[0](left, i), ag_r.at[turn, i]

    def from_right(plan, turn, i):
        return plan[0](right, i), ag_r.at[turn, grps + i]

    def gather_forward(plan, turn, i):
        _, send, far = plan
        if i % 2:
            arrive("w_near", from_right(plan, turn, i))
            send(right, i, far[i], to_left)
        else:
            arrive("w_near", from_left(plan, turn, i))
            send(left, i, far[i], to_right)

    gathered = gather_plan(tb, 0)
    for i in range(0, grps, 2):
        gather_send(gathered, i)
    gather_rest(gathered)

    def spread_news(step):
        for i, pair in enumerate((line, plane)):
            for where in pair:
                pl.semaphore_signal(
                    news.at[i, step], inc=1, device_id=where, device_id_type=MESH
                )

    def take_news(step):
        with jax.named_scope("w_news"):
            for i in range(2):
                pl.semaphore_wait(news.at[i, step], 2)

    spread_news(0)

    for load in loads[1:6]:
        load.wait()
    stacked = jnp.concatenate(
        [own_tab[...].astype(F32), mor_tab[...].astype(F32), ver_tab[...].astype(F32)], axis=0
    ).astype(BF16)
    placed = jnp.where(
        iota((subs, subs), 0) == jnp.broadcast_to(hol_tab[...], (subs, subs)), 1.0, 0.0
    ).astype(BF16)
    moved = dot_nn(stacked, placed)
    faces = own_tab.shape[0]
    held_all, mortar_all = moved[:faces], moved[faces : 2 * faces]
    vertex_all = moved[2 * faces :]

    def column(table, index):
        mask = iota(table.shape, 1) == index
        return jnp.sum(jnp.where(mask, table, 0.0), axis=1, keepdims=True)

    square_i, square_j = iota((faces, faces), 0), iota((faces, faces), 1)

    def as_row(col):
        return jnp.sum(jnp.where(square_i == square_j, col, 0.0), axis=0, keepdims=True)

    held_c = column(held_all, s)
    held_r = as_row(held_c)
    rank_r = jnp.sum(
        jnp.where((held_c == held_r) & (square_i < square_j), 1.0, 0.0), axis=0, keepdims=True
    )
    slot_r = held_r * CAP + rank_r
    rows = iota((wm.shape[0], faces), 0)
    face_of = jnp.left_shift(jnp.right_shift(rows, 7), 3) | (rows & 7)
    slot_c = jnp.sum(
        jnp.where(iota(rows.shape, 1) == face_of, slot_r, 0.0), axis=1, keepdims=True
    )
    r_i, c_i = iota(wm.shape, 0), iota(wm.shape, 1)
    same = (jnp.right_shift(r_i, 3) & 15) == (jnp.right_shift(c_i, 3) & 15)
    slot_of = (jnp.left_shift(jnp.right_shift(c_i, 7), 3) | (c_i & 7)).astype(F32)
    wm[...] = jnp.where(same & (slot_c == slot_of), 1.0, 0.0).astype(BF16)

    width = vm.shape[1]
    lane8 = iota((faces, CAP), 1).astype(F32)
    pick8 = iota((LANES, CAP), 1) == (iota((LANES, CAP), 0) & 7)
    v_r, v_c = iota((LANES, width), 0), iota((LANES, width), 1)
    v_same = jnp.right_shift(v_r, 3) == jnp.right_shift(v_c, 4)
    v_key = (v_c & 15).astype(F32)
    counts = jnp.zeros((1, width), F32)
    for link in range(LINKS):
        sender = sub_at(REACH - link)
        hc, mc = column(held_all, sender), column(mortar_all, sender)
        hr = as_row(hc)
        rank_c = jnp.sum(
            jnp.where((hr == hc) & (square_j < square_i), 1.0, 0.0), axis=1, keepdims=True
        )
        key8 = (
            jnp.sum(
                jnp.where((hc == float(link)) & (rank_c == lane8), mc + 1.0, 0.0),
                axis=0,
                keepdims=True,
            )
            - 1.0
        )
        key_c = jnp.sum(jnp.where(pick8, key8, 0.0), axis=1, keepdims=True)
        block = jnp.where(v_same & (key_c == v_key), 1.0, 0.0)
        counts = counts + jnp.sum(block, axis=0, keepdims=True)
        vm[pl.ds(link * LANES, LANES), :] = block.astype(BF16)
    order_c = column(ord_tab[...].astype(F32), s)
    order_r = jnp.sum(
        jnp.where(iota((MORT_OWN, width), 0) == (iota((MORT_OWN, width), 1) & 15), order_c, 0.0),
        axis=0,
        keepdims=True,
    )
    inverse = 1.0 / jnp.maximum(counts, 1.0)
    row_c = iota((1, width), 1)
    for mg in range(4):
        first = (2 * mg + jnp.right_shift(row_c, 7)).astype(F32)
        second = (jnp.right_shift(row_c, 4) & 7).astype(F32)
        keep = (first <= order_r) & (second <= order_r)
        fac[pl.ds(mg, 1), :] = jnp.where(keep, inverse, 0.0)

    vertex_b = vertex_all.astype(BF16)
    d_rows, d_cols = dm.shape[0] // 2, dm.shape[1]
    here = jnp.where(
        iota((d_rows, subs), 1) == z * yc_n + jnp.right_shift(iota((d_rows, subs), 0), 3), 1.0, 0.0
    ).astype(BF16)
    wanted = dot_nt(here, vertex_b)
    wanted = jnp.sum(
        jnp.where(iota((d_rows, NCV), 1) == (iota((d_rows, NCV), 0) & 7), wanted, 0.0),
        axis=1,
        keepdims=True,
    )
    block = zs_n * NCV
    places = iota((subs, block), 0)
    corner = iota((subs, block), 1)
    met = []
    for link in range(LINKS):
        sender = jnp.right_shift(corner, 3) * yc_n + yc + (subs + REACH - link)
        there = jnp.where(places == (sender & (subs - 1)), 1.0, 0.0).astype(BF16)
        given = dot_nn(vertex_b, there)
        given = jnp.sum(
            jnp.where(iota((NCV, block), 0) == (iota((NCV, block), 1) & 7), given, 0.0),
            axis=0,
            keepdims=True,
        )
        met.append(jnp.where(wanted == given, 1.0, 0.0))
    met.append(jnp.zeros_like(met[0]))
    for i in range(HALF_LINKS):
        for side in range(2):
            dm[pl.ds(side * d_rows, d_rows), pl.ds(i * block, block)] = met[
                side * HALF_LINKS + i
            ].astype(BF16)

    lane = iota((CAP, LANES), 1)
    row8 = iota((CAP, 4 * LANES), 0)
    own_face = row8 == jnp.right_shift(iota((CAP, 4 * LANES), 1), 6)

    def build_block(q):
        def step(i, carry):
            pair = pa[q, :, pl.ds(pl.multiple_of(i * LANES, LANES), LANES)].astype(F32)
            turned = pltpu.roll(pair, LANES // 2, 1)
            even = jnp.where(lane < LANES // 2, pair, turned)
            odd = jnp.where(lane < LANES // 2, turned, pair)
            even = jnp.where(own_face, jnp.concatenate([even] * 4, axis=1), 0.0)
            odd = jnp.where(own_face, jnp.concatenate([odd] * 4, axis=1), 0.0)
            both = jnp.concatenate([even, odd], axis=0).astype(BF16)
            bd[q, pl.ds(pl.multiple_of(i * 16, 16), 16), :] = both
            return carry

        lax.fori_loop(0, pa.shape[2] // LANES, step, 0, unroll=8)

    def fold_block(q, s_block):
        wide = dot_nt(s_block, bd[q]).astype(BF16)
        for mg in range(4):
            sp[mg, :, pl.ds(pl.multiple_of(q * LANES, LANES), LANES)] = wide[
                :, mg * LANES : (mg + 1) * LANES
            ]

    def fold_coarse():
        both = jnp.concatenate(halves(dot_nt(ca[g], bd[g])), axis=0)
        for mg in range(4):
            qm[g, pl.ds(mg * 2 * NCV, 2 * NCV), :] = both[:, mg * LANES : (mg + 1) * LANES]

    loads[6].wait()
    loads[7].wait()
    with jax.named_scope("c_block"):
        build_block(g)
    take_news(0)
    spread_news(1)
    with jax.named_scope("w_loads"):
        for load in loads[8:]:
            load.wait()
    for i in range(grps):
        gather_forward(gathered, 0, i)
        if i == 1:
            take_news(1)
            spread_news(2)
    take_news(2)
    fold_coarse()
    for i, ref in enumerate((ca, qm)):
        for step in (2, 1, 3):
            where = {"grp": grp_at(step)}
            remote(ref.at[g], ref.at[g], p_s.at[i], p_r.at[i], where).start()

    def add_block(q):
        acc[...] += dot_nt(tb[q], s4[q])

    acc[...] = dot_nt(tb[g], s4[g])
    arrive("w_left", from_left(gathered, 0, 1), from_left(gathered, 0, 3))
    add_block(left)
    arrive("w_right", from_right(gathered, 0, 0), from_right(gathered, 0, 2))
    add_block(right)
    arrive("w_across", (tb.at[across], ag_r.at[0, 2 * grps]))
    add_block(across)
    prod[...] = acc[...] - rh[...]

    groups = 4 // PARTS
    span = groups * quarter

    def rows_of(part):
        return pl.ds(part * span, span)

    def swap_out(turn, part, q):
        remote(
            sb.at[turn, q, rows_of(part)],
            ar.at[turn, g, rows_of(part)],
            a2a_s.at[turn],
            a2a_r.at[turn, part],
            {"grp": q},
        ).start()

    def swap_all(residual):
        residual = residual.astype(BF16)
        for part in range(PARTS):
            first = part * groups
            modes = bd[g, pl.ds(first * LANES, groups * LANES), :]
            coeffs = dot_nt(residual, modes).astype(BF16)
            for q in range(grps):
                for mg in range(groups):
                    sb[0, q, pl.ds((first + mg) * quarter, quarter), :] = coeffs[
                        q * quarter : (q + 1) * quarter, mg * LANES : (mg + 1) * LANES
                    ]
            for step in (2, 1, 3):
                swap_out(0, part, grp_at(step))
        ar[0, g] = sb[0, g]

    def swap_quarter(q, own):
        at = pl.ds(pl.multiple_of(q * quarter, quarter), quarter)
        coeffs = dot_nt(acc[at, :].astype(BF16), bd[g]).astype(BF16)
        tall = jnp.concatenate(
            [coeffs[:, mg * LANES : (mg + 1) * LANES] for mg in range(4)], axis=0
        )
        if own:
            ar[1, g] = tall
            return
        sb[1, q] = tall
        for part in range(PARTS):
            swap_out(1, part, q)

    def exchange(turn, picked, deliver):
        partials = []
        if turn == 0:
            for step in (2, 1, 3):
                where = {"grp": grp_at(step)}
                remote(pa.at[g], pa.at[g], p_s.at[4], p_r.at[4], where).start()
            others = pl.ds(0, grps - 1)
            fold_block(g, s4[g])
            arrive("w_extra", (ca.at[others], p_r.at[0]), (qm.at[others], p_r.at[1]))
            slots = dot_nn(
                jnp.concatenate([qm[q] for q in range(grps)], axis=1), wm[...]
            ).astype(BF16)
            for link in (0, 4, 1, 3, 2):
                piece = slots[:, link * LANES : (link + 1) * LANES]
                if link == REACH:
                    qr[link] = piece
                    continue
                qs[link] = piece
        terms = None if picked is None else picked()
        for part in range(PARTS):
            arrive("w_a2a", (ar.at[turn, pl.ds(0, grps - 1), rows_of(part)], a2a_r.at[turn, part]))
            lines = [ar[turn, q, rows_of(part), :] for q in range(grps)]
            if terms is not None:
                for q in range(grps):
                    tall = jnp.concatenate(
                        [
                            terms[q][:, mg * LANES : (mg + 1) * LANES]
                            for mg in range(part * groups, (part + 1) * groups)
                        ],
                        axis=0,
                    )
                    lines[q] = (lines[q].astype(F32) - coarse_weight * tall).astype(BF16)
            grouped = dot_nn(jnp.concatenate(lines, axis=1), wm[...]).astype(BF16)
            for link in (0, 4, 1, 3, 2):
                piece = grouped[:, link * LANES : (link + 1) * LANES]
                if link == REACH:
                    orr[turn, link, rows_of(part), :] = piece
                    continue
                zs[turn, link, rows_of(part), :] = piece
                remote(
                    zs.at[turn, link, rows_of(part)],
                    orr.at[turn, link, rows_of(part)],
                    ex_s.at[turn],
                    ex_r.at[turn, part],
                    {"sub": sub_at(link - REACH)},
                ).start()
        if turn == 0:
            for link in (0, 4, 1, 3):
                where = {"sub": sub_at(link - REACH)}
                remote(qs.at[link], qr.at[link], p_s.at[3], p_r.at[3], where).start()
            arrive("w_p", (pa.at[others], p_r.at[4]))
            for i in range(grps - 1):
                build_block(grp_at(i + 1))
        for part in range(PARTS):
            arrive("w_ex", (orr.at[turn, pl.ds(0, LINKS - 1), rows_of(part)], ex_r.at[turn, part]))
            joined = jnp.concatenate(
                [orr[turn, link, rows_of(part), :] for link in range(LINKS)], axis=1
            )
            sums = dot_nn(joined, vm[...])
            averages = jnp.concatenate(
                [
                    sums[mg * quarter : (mg + 1) * quarter]
                    * fac[pl.ds(part * groups + mg, 1), :]
                    for mg in range(groups)
                ],
                axis=0,
            ).astype(BF16)
            replies = dot_nt(averages, vm[...]).astype(BF16)
            for link in (0, 4, 1, 3, 2):
                piece = replies[:, link * LANES : (link + 1) * LANES]
                if link == REACH:
                    rr[turn, link, rows_of(part), :] = piece
                    continue
                rs[turn, link, rows_of(part), :] = piece
                remote(
                    rs.at[turn, link, rows_of(part)],
                    rr.at[turn, link, rows_of(part)],
                    ret_s.at[turn],
                    ret_r.at[turn, part],
                    {"sub": sub_at(REACH - link)},
                ).start()
            if turn == 0:
                av[rows_of(part), :] = averages
            else:
                partials.append(coarse_part(part, averages))
        if turn == 1:
            coarse_first(1, sum(partials[1:], partials[0]))
            lift_first()
            coarse_second(1)
        if turn == 0:
            arrive("w_q", (qr.at[pl.ds(0, LINKS - 1)], p_r.at[3]))
            build_owner()
            partials = [coarse_part(part, av[rows_of(part), :]) for part in range(PARTS)]
            coarse_first(0, sum(partials[1:], partials[0]))
            for i in range(grps - 1):
                q = grp_at(i + 1)
                fold_block(q, s4[q])
            spread = dot_nt(ca[0], s4[0])
            for q in range(1, grps):
                spread = spread + dot_nt(ca[q], s4[q])
            high, rest = halves(spread)
            psc[g] = jnp.concatenate(
                halves(dot_nt(high, bd[g]) + dot_nt(rest, bd[g])), axis=0
            )
            for step in (2, 1, 3):
                where = {"grp": grp_at(step)}
                remote(psc.at[g], psc.at[g], p_s.at[2], p_r.at[2], where).start()
        for part in range(PARTS):
            arrive("w_ret", (rr.at[turn, pl.ds(0, LINKS - 1), rows_of(part)], ret_r.at[turn, part]))
            answered = jnp.concatenate(
                [rr[turn, link, rows_of(part), :] for link in range(LINKS)], axis=1
            )
            deliver(part, dot_nt(answered, wm[...]).astype(BF16))

    def build_owner():
        lines = []
        for link in range(LINKS):
            both = dot_nn(qr[link], vm[pl.ds(link * LANES, LANES), :])
            lines.append(
                [
                    both[mg * 2 * NCV : mg * 2 * NCV + NCV]
                    + both[mg * 2 * NCV + NCV : (mg + 1) * 2 * NCV]
                    for mg in range(4)
                ]
            )
        for mg in range(4):
            full = jnp.concatenate([line[mg] for line in lines], axis=0)
            gm[mg] = jnp.concatenate(halves(full), axis=0)

    def coarse_part(part, averages):
        gap = jnp.zeros((LANES // 2 - quarter, averages.shape[1]), BF16)
        total = None
        for mg in range(groups):
            line = averages[mg * quarter : (mg + 1) * quarter]
            twice = jnp.concatenate([line, gap, line, gap], axis=0)
            value = dot_nt(gm[part * groups + mg], twice)
            total = value if total is None else total + value
        return total[: LINKS * NCV] + total[LINKS * NCV :]

    side = iota((HALF_LINKS * NCV, LANES), 1) < LANES // 2

    def coarse_first(turn, value):
        first = value[: HALF_LINKS * NCV]
        second = jnp.concatenate(
            [value[HALF_LINKS * NCV :], jnp.zeros((NCV, LANES), F32)], axis=0
        )
        ps[turn] = jnp.where(side, first, second).astype(BF16)
        for step in range(zs_n - 1):
            to = lax.rem(z + step + 1, zs_n) * yc_n + yc
            remote(
                ps.at[turn], pz.at[turn, z], k1_s.at[turn], k1_r.at[turn], {"sub": to}
            ).start()
        pz[turn, z] = ps[turn]

    def coarse_second(turn):
        arrive("w_k1", (pz.at[turn, pl.ds(0, zs_n - 1)], k1_r.at[turn]))
        near = pz[turn].astype(F32)
        lines = jnp.concatenate(
            [
                near[:, i * NCV : (i + 1) * NCV, :].reshape(zs_n * NCV, LANES)
                for i in range(HALF_LINKS)
            ],
            axis=0,
        ).astype(BF16)
        value = dot_nn(dm[...], lines)
        half_rows = value.shape[0] // 2
        lane_of = iota((half_rows, LANES), 1)
        value = jnp.where(lane_of < LANES // 2, value[:half_rows], value[half_rows:])
        ks[turn] = value.reshape(yc_n, NCV, LANES)
        for step in range(yc_n - 1):
            to = lax.rem(yc + step + 1, yc_n)
            remote(
                ks.at[turn, to],
                kr.at[turn, yc],
                k2_s.at[turn],
                k2_r.at[turn],
                {"sub": z * yc_n + to},
            ).start()
        kr[turn, yc] = ks[turn, yc]

    def coarse_third(turn):
        arrive("w_k2", (kr.at[turn, pl.ds(0, yc_n - 1)], k2_r.at[turn]))
        total = jnp.sum(kr[turn], axis=0)
        return total + pltpu.roll(total, LANES // 2, 1)

    gathered = gather_plan(af, 1)
    def spread_out(part, mine):
        af[g, rows_of(part), :] = mine
        for i in range(part * groups, (part + 1) * groups, 2):
            gather_send(gathered, i)
        if part == PARTS - 1:
            gather_rest(gathered)

    swap_all(prod[...])
    exchange(0, None, spread_out)

    def add_modes(q, groups_of, fresh):
        at = pl.ds(pl.multiple_of(q * quarter, quarter), quarter)
        value = dot_nt(af[q, pl.ds(groups_of[0] * quarter, quarter), :], sp[groups_of[0]])
        for mg in groups_of[1:]:
            value = value + dot_nt(af[q, pl.ds(mg * quarter, quarter), :], sp[mg])
        base = prod if fresh else acc
        acc[at, :] = base[at, :] - relax_weight * value

    add_modes(g, (0, 1, 2, 3), True)
    swap_quarter(g, True)
    for i in range(grps):
        gather_forward(gathered, 1, i)
    coarse_second(0)
    arrive("w_left", from_left(gathered, 1, 1))
    add_modes(left, (0, 1), True)
    arrive("w_right", from_right(gathered, 1, 0))
    add_modes(right, (0, 1), True)
    arrive("w_left", from_left(gathered, 1, 3))
    add_modes(left, (2, 3), False)
    swap_quarter(left, False)
    arrive("w_right", from_right(gathered, 1, 2))
    add_modes(right, (2, 3), False)
    swap_quarter(right, False)
    for part in range(2):
        far = af.at[across, pl.ds(2 * part * quarter, 2 * quarter)]
        arrive("w_across", (far, ag_r.at[1, 2 * grps + part]))
        add_modes(across, (2 * part, 2 * part + 1), part == 0)
    swap_quarter(across, False)
    totals = []

    def first_picked():
        arrive("w_psc", (psc.at[pl.ds(0, grps - 1)], p_r.at[2]))
        picked = coarse_third(0)
        totals.append(picked)
        high, rest = halves(picked.T[:quarter])
        both = jnp.concatenate(
            [jnp.concatenate([high, high], axis=1), jnp.concatenate([rest, rest], axis=1)],
            axis=0,
        )
        terms = []
        for q in range(grps):
            term = dot_nn(both, psc[q])
            terms.append(term[:quarter] + term[quarter:])
        return terms

    def hand_back(part, mine):
        for q in range(grps):
            ls[q, rows_of(part), :] = mine[:, q * LANES : (q + 1) * LANES]
        for step in (2, 1, 3):
            to = grp_at(step)
            remote(
                ls.at[to, rows_of(part)], lr.at[g, rows_of(part)], fin_s, fin_r, {"grp": to}
            ).start()

    def own_rows(blocks):
        lines = [
            jnp.concatenate(
                [block[mg * quarter : (mg + 1) * quarter] for mg in range(4)], axis=1
            )
            for block in blocks
        ]
        return jnp.concatenate(lines, axis=0)

    def lift_first():
        here = pl.ds(pl.multiple_of(g * LANES, LANES), LANES)
        lifted = dot_nn(own_rows([af[q, :, here] for q in range(grps)]), bd[g])
        acc[...] = st[...] - relax_weight * lifted

    exchange(1, first_picked, hand_back)
    lr[g] = ls[g]
    pk[g] = coarse_third(1) + totals[0]
    for step in (2, 1, 3):
        remote(pk.at[g], pk.at[g], k3_s, k3_r, {"grp": grp_at(step)}).start()
    arrive("w_fin", (lr.at[pl.ds(0, grps - 1)], fin_r))
    acc[...] -= relax_weight * dot_nn(own_rows([lr[q] for q in range(grps)]), bd[g])
    basis = jnp.concatenate([ca[g], ca[g]], axis=0)
    arrive("w_k3", (pk.at[pl.ds(0, grps - 1)], k3_r))
    tall = jnp.concatenate([pk[q].T[:quarter] for q in range(grps)], axis=0)
    corr = dot_nn(jnp.concatenate(halves(tall), axis=1), basis)
    out[...] = acc[...] - coarse_weight * corr

    others = pl.ds(0, grps - 1)
    done = [
        (tb.at[others], ag_s.at[0]),
        (af.at[others], ag_s.at[1]),
        (ca.at[others], p_s.at[0]),
        (qm.at[others], p_s.at[1]),
        (pa.at[others], p_s.at[4]),
        (psc.at[others], p_s.at[2]),
        (qs.at[pl.ds(0, LINKS - 1)], p_s.at[3]),
        (ls.at[others], fin_s),
        (pk.at[others], k3_s),
    ]
    for turn in range(ITERS):
        done += [
            (sb.at[turn, others], a2a_s.at[turn]),
            (zs.at[turn, pl.ds(0, LINKS - 1)], ex_s.at[turn]),
            (rs.at[turn, pl.ds(0, LINKS - 1)], ret_s.at[turn]),
            (pz.at[turn, pl.ds(0, zs_n - 1)], k1_s.at[turn]),
            (ks.at[turn, pl.ds(0, yc_n - 1)], k2_s.at[turn]),
        ]
    with jax.named_scope("w_sends"):
        for ref, sem in done:
            whole(ref, sem).wait_send()


def solution(mesh):
    subs, grps = mesh.shape["sub"], mesh.shape["grp"]
    zs_n = 8 if subs == 128 else 2
    yc_n = subs // zs_n
    sizes = (subs, grps, zs_n, yc_n)

    def body(
        schur,
        rhs,
        start,
        project,
        coarse_basis,
        owner_of_face,
        mortar_of_face,
        mortar_order,
        subdomain_map,
        vertex_ids,
    ):
        rows, cols = schur.shape[1], schur.shape[2]
        part = cols // grps
        wide = rhs.shape[2]
        faces = owner_of_face.shape[1]
        block = LANES
        dma = pltpu.SemaphoreType.DMA
        vmem = pltpu.VMEM
        scratch = [
            vmem((grps, rows, part), BF16),
            vmem((wide, rows), F32),
            vmem((wide, rows), F32),
            vmem((grps, wide, rows), BF16),
            vmem((grps, wide, rows), BF16),
            vmem((grps,) + project.shape[1:], BF16),
            vmem((grps,) + coarse_basis.shape[1:], BF16),
            vmem((grps, rows, rows), BF16),
            vmem((4, rows, rows), BF16),
            vmem((rows, LINKS * block), BF16),
            vmem((LINKS * block, 16 * MORT_OWN), BF16),
            vmem((8, 16 * MORT_OWN), F32),
            vmem((wide, rows), F32),
            vmem((wide, rows), F32),
            vmem((ITERS, grps, wide, block), BF16),
            vmem((ITERS, grps, wide, block), BF16),
            vmem((ITERS, LINKS, wide, block), BF16),
            vmem((ITERS, LINKS, wide, block), BF16),
            vmem((ITERS, LINKS, wide, block), BF16),
            vmem((ITERS, LINKS, wide, block), BF16),
            vmem((grps, wide, block), BF16),
            vmem((grps, wide, block), BF16),
            vmem((grps, 8 * NCV, block), BF16),
            vmem((LINKS, 8 * NCV, block), BF16),
            vmem((LINKS, 8 * NCV, block), BF16),
            vmem((4, 2 * LINKS * NCV, 16 * MORT_OWN), BF16),
            vmem((wide, 16 * MORT_OWN), BF16),
            vmem((grps, 2 * NCV, rows), BF16),
            vmem((2 * yc_n * NCV, HALF_LINKS * zs_n * NCV), BF16),
            vmem((ITERS, HALF_LINKS * NCV, LANES), BF16),
            vmem((ITERS, zs_n, HALF_LINKS * NCV, LANES), BF16),
            vmem((ITERS, yc_n, NCV, LANES), F32),
            vmem((ITERS, yc_n, NCV, LANES), F32),
            vmem((grps, NCV, LANES), F32),
            vmem((faces, subs), jnp.int32),
            vmem((faces, subs), jnp.int32),
            vmem((MORT_OWN, subs), jnp.int32),
            vmem((1, subs), jnp.int32),
            vmem((NCV, subs), jnp.int32),
            dma((9 + grps,)),
            dma((2,)),
            dma((2, 2 * grps + 2)),
            dma((ITERS,)),
            dma((ITERS, PARTS)),
            dma((ITERS,)),
            dma((ITERS, PARTS)),
            dma((ITERS,)),
            dma((ITERS, PARTS)),
            dma((5,)),
            dma((5,)),
            dma((ITERS,)),
            dma((ITERS,)),
            dma((ITERS,)),
            dma((ITERS,)),
            dma(()),
            dma(()),
            dma(()),
            dma(()),
            pltpu.SemaphoreType.REGULAR((2, 3)),
        ]
        operands = (
            schur[0],
            rhs[0].T,
            start[0].T,
            project[0],
            coarse_basis[0],
            owner_of_face[:, :, 0].T,
            mortar_of_face.T,
            mortar_order.T,
            subdomain_map.reshape(1, subs),
            vertex_ids.T,
        )
        result = pl.pallas_call(
            functools.partial(kernel, sizes),
            out_shape=jax.ShapeDtypeStruct((wide, rows), F32),
            in_specs=[pl.BlockSpec(memory_space=pltpu.HBM)] * 10,
            out_specs=pl.BlockSpec(memory_space=pltpu.VMEM),
            scratch_shapes=scratch,
            compiler_params=pltpu.CompilerParams(
                collective_id=0, has_side_effects=True, vmem_limit_bytes=44 * 1024 * 1024
            ),
        )(*(pltpu.with_memory_space_constraint(value, pltpu.HBM) for value in operands))
        return result.T[None]

    split = P("sub", "grp", None)
    return jax.shard_map(
        body,
        mesh=mesh,
        in_specs=(split, split, split, split, P("sub", None, "grp"), P(), P(), P(), P(), P()),
        out_specs=split,
        check_vma=False,
    )
```
